256 devices in a mesh: seq: 32 (over z, x), head: 8 (over y, core).
Axes of the slice: x: 4, y: 4, z: 8, core: 2. Of those that a mesh axis runs over, the one named last changes fastest.
Arguments:
- queries: bfloat16 [16384, 1024], P('seq', 'head'), may hold values from -6 to 6
- keys: bfloat16 [16384, 1024], P('seq', 'head'), may hold values from -5 to 5
- values: bfloat16 [16384, 1024], P('seq', 'head'), may hold values from -6 to 6
- ridge: float32 [8], P('head'), may hold values from 0.5 to 4
- gain: float32 [1024], P('head'), may hold values from 0.5 to 1.5
- grad_out: bfloat16 [16384, 1024], P('seq', 'head'), may hold values from -6 to 6
Outputs:
- output: bfloat16 [16384, 1024], P('seq', 'head')
- grad_queries: bfloat16 [16384, 1024], P('seq', 'head')
- grad_keys: bfloat16 [16384, 1024], P('seq', 'head')
- grad_values: bfloat16 [16384, 1024], P('seq', 'head')
- grad_gain: float32 [1024], P('head')
The draws below stay inside these ranges and needn't reach their ends.
All inputs are finite; a program needn't handle non-finite values.
Results may differ from the reference program's by a relative error of at most 0.0044.
Values sent between devices are 32-bit elements; how exact they have to be, the bound alone decides.
No kernel may reach another device: no remote copies, remote signals or barrier semaphores. Data moves between devices by JAX's collectives and lax.ppermute only.
A program may use at most 64 MiB of HBM per device.

```python
import math
import jax
import jax.numpy as jnp
from jax import lax

HEADS = 8
D = 128
TOK_DEV = 512
CG_STEPS = 6
TOKENS = 16384


def draw_keys(key, part):
    first, second = jax.random.split(jax.random.fold_in(key, 17))
    scales = jnp.exp(jax.random.uniform(first, (HEADS * D,), jnp.float32, math.log(0.05), 0.0))
    noise = jnp.clip(jax.random.normal(second, (TOKENS, HEADS * D), jnp.float32), -5.0, 5.0)
    return (noise * scales[None, :]).astype(jnp.bfloat16)


def level_of(stream_key, dims, cuts, least, top_value):
    def one(dim, parts):
        steps = jax.random.uniform(jax.random.fold_in(jax.random.fold_in(stream_key, 6), dim), (parts,), jnp.float32, least / len(cuts), top_value / len(cuts))
        return jnp.repeat(jnp.exp(steps), dims[dim] // parts).reshape((-1,) + (1,) * (len(dims) - dim - 1))

    loudness = one(*cuts[0])
    for cut in cuts[1:]:
        loudness = loudness * one(*cut)
    return loudness


def scatter_about(own_key, dims, deviation, limit, pieces=(), held_as=jnp.bfloat16):
    level = level_of(own_key, dims, pieces, -0.22, 0.18) if pieces else 1.0
    drawn = jax.random.normal(own_key, dims, jnp.float32) * deviation * level
    return jnp.minimum(jnp.maximum(drawn, -limit), limit).astype(held_as)


def setup_inputs(seed: int = 0) -> dict:
    arg_keys = jax.random.split(jax.random.key(seed), 7)
    queries = scatter_about(arg_keys[0], (TOKENS, HEADS * D), 1.0, 6.0, ((0, 32), (1, 8)))
    keys = draw_keys(jax.random.fold_in(arg_keys[6], 71), 0)
    values = scatter_about(arg_keys[2], (TOKENS, HEADS * D), 1.0, 6.0, ((0, 32), (1, 8)))
    ridge = jnp.clip(jnp.exp(math.log(4.0) - 2.0794415 * jax.random.uniform(arg_keys[3], (HEADS,), jnp.float32) ** level_of(arg_keys[3], (HEADS,), ((0, 8),), -0.2, 0.2)), 0.5, 4.0)
    gain = jnp.clip(1.0 + 0.1 * jax.random.normal(arg_keys[4], (HEADS * D,), jnp.float32), 0.5, 1.5)
    grad_out = scatter_about(arg_keys[5], (TOKENS, HEADS * D), 1.0, 6.0, ((0, 32), (1, 8)))
    return dict(queries=queries, keys=keys, values=values, ridge=ridge, gain=gain, grad_out=grad_out)


EPS = 1e-06
HIGH = lax.Precision.HIGHEST

def matmul(left, right):
    return jnp.dot(left, right, precision=HIGH)

def rows_by_rows(left, right):
    return lax.dot_general(left, right, (((1,), (1,)), ((), ())), precision=HIGH)

def cols_by_cols(left, right):
    return lax.dot_general(left, right, (((0,), (0,)), ((), ())), precision=HIGH)

def lower_mask(count):
    rows = lax.broadcasted_iota(jnp.int32, (count, count), 0)
    cols = lax.broadcasted_iota(jnp.int32, (count, count), 1)
    return (rows >= cols).astype(jnp.float32)

def conjugate(apply_fn, rhs):
    solution = jnp.zeros_like(rhs)
    resid = rhs
    search = rhs
    norm_now = lax.optimization_barrier(jnp.sum(resid * resid, axis=-1, keepdims=True))
    for _ in range(CG_STEPS):
        image = apply_fn(search)
        alpha = norm_now / (lax.optimization_barrier(jnp.sum(search * image, axis=-1, keepdims=True)) + EPS)
        solution = solution + alpha * search
        resid = resid - alpha * image
        norm_next = lax.optimization_barrier(jnp.sum(resid * resid, axis=-1, keepdims=True))
        search = resid + norm_next / (norm_now + EPS) * search
        norm_now = norm_next
    return solution

def make_apply(gram_prev, keys_blk, ridge, mask):

    def apply_fn(search):
        return matmul(search, gram_prev) + matmul(mask * rows_by_rows(search, keys_blk), keys_blk) + ridge * search
    return apply_fn

def forward_block(queries_blk, keys_blk, values_blk, gram_prev, assoc_prev, ridge):
    mask = lower_mask(queries_blk.shape[0])
    solved = conjugate(make_apply(gram_prev, keys_blk, ridge, mask), queries_blk)
    mixed = rows_by_rows(solved, assoc_prev) + matmul(mask * rows_by_rows(solved, keys_blk), values_blk)
    return (solved, mixed)

def adjoint_block(keys_blk, values_blk, gram_prev, assoc_prev, ridge, solved, grad_mixed):
    mask = lower_mask(keys_blk.shape[0])
    rhs = matmul(grad_mixed, assoc_prev) + matmul(mask * rows_by_rows(grad_mixed, values_blk), keys_blk)
    adjoint = conjugate(make_apply(gram_prev, keys_blk, ridge, mask), rhs)
    suffix_loc = cols_by_cols(grad_mixed, solved)
    pair = cols_by_cols(adjoint, solved)
    return (adjoint, suffix_loc, pair + pair.T)

def grads_block(keys_blk, values_blk, solved, adjoint, grad_mixed, suffix_next, pairs_next):
    upper = lower_mask(keys_blk.shape[0]).T
    key_solved = upper * rows_by_rows(keys_blk, solved)
    grad_values = rows_by_rows(keys_blk, suffix_next) + matmul(key_solved, grad_mixed)
    grad_keys = matmul(values_blk, suffix_next) + matmul(upper * rows_by_rows(values_blk, grad_mixed), solved) - matmul(keys_blk, pairs_next) - matmul(key_solved, adjoint) - matmul(upper * rows_by_rows(keys_blk, adjoint), solved)
    return (grad_keys, grad_values)

def to_heads(array):
    blocks = TOKENS // TOK_DEV
    return jnp.transpose(array.astype(jnp.float32).reshape(TOKENS, HEADS, D), (1, 0, 2)).reshape(HEADS, blocks, TOK_DEV, D)

def from_heads(array):
    return jnp.transpose(array.reshape(HEADS, TOKENS, D), (1, 0, 2)).reshape(TOKENS, HEADS * D)

def reference(queries, keys, values, ridge, gain, grad_out):
    query_h = to_heads(queries)
    key_h = to_heads(keys)
    value_h = to_heads(values)
    zeros = jnp.zeros((D, D), jnp.float32)

    def forward_head(items):
        query_b, key_b, value_b, ridge_one = items

        def step_fn(carry, blk):
            gram, assoc = carry
            query_blk, key_blk, value_blk = blk
            solved, mixed = forward_block(query_blk, key_blk, value_blk, gram, assoc, ridge_one)
            new = (gram + cols_by_cols(key_blk, key_blk), assoc + cols_by_cols(value_blk, key_blk))
            return (new, (solved, mixed, gram, assoc))
        _, outs = lax.scan(step_fn, (zeros, zeros), (query_b, key_b, value_b))
        return outs
    solved, mixed, grams, assocs = lax.map(forward_head, (query_h, key_h, value_h, ridge))
    squares = lax.optimization_barrier(jnp.sum(mixed * mixed, axis=(0, 3)))
    denom = jnp.sqrt(squares / (HEADS * D) + EPS)[None, :, :, None]
    gains = gain.reshape(HEADS, 1, 1, D)
    output = from_heads(mixed * gains / denom).astype(jnp.bfloat16)
    upstream = to_heads(grad_out)
    grad_gain = lax.optimization_barrier(jnp.sum(upstream * mixed / denom, axis=(1, 2))).reshape(HEADS * D)
    centre = lax.optimization_barrier(jnp.sum(gains * upstream * mixed, axis=(0, 3)))[None, :, :, None]
    grad_mixed = gains * upstream / denom - mixed * centre / (denom ** 3 * (HEADS * D))

    def backward_head(items):
        key_b, value_b, gram_b, assoc_b, ridge_one, solved_b, grad_b = items

        def step_fn(carry, blk):
            suffix_next, pairs_next = carry
            key_blk, value_blk, gram, assoc, solved_blk, grad_blk = blk
            adjoint, suffix_loc, pair_loc = adjoint_block(key_blk, value_blk, gram, assoc, ridge_one, solved_blk, grad_blk)
            grad_keys, grad_values = grads_block(key_blk, value_blk, solved_blk, adjoint, grad_blk, suffix_next, pairs_next)
            return ((suffix_next + suffix_loc, pairs_next + pair_loc), (adjoint, grad_keys, grad_values))
        _, outs = lax.scan(step_fn, (zeros, zeros), (key_b, value_b, gram_b, assoc_b, solved_b, grad_b), reverse=True)
        return outs
    adjoint, grad_keys, grad_values = lax.map(backward_head, (key_h, value_h, grams, assocs, ridge, solved, grad_mixed))
    return (output, from_heads(adjoint).astype(jnp.bfloat16), from_heads(grad_keys).astype(jnp.bfloat16), from_heads(grad_values).astype(jnp.bfloat16), grad_gain)
```

```python
import jax
import jax.numpy as jnp
from jax import lax
from jax.experimental import pallas as pl
from jax.experimental.pallas import tpu as pltpu
from jax.sharding import Mesh
from jax.sharding import PartitionSpec as P

HEADS = 8
D = 128
CG_STEPS = 6
EPS = 1e-06
ZN = 8
XN = 4
SEQ = ("z", "x")
C = 128
F32 = jnp.float32
BF16 = jnp.bfloat16
VMEM = pl.BlockSpec(memory_space=pltpu.VMEM)
SMEM = pl.BlockSpec(memory_space=pltpu.SMEM)


def split2(x):
    high = x.astype(BF16)
    return high, (x - high.astype(F32)).astype(BF16)


def mm(left, right):
    return jnp.dot(left, right, preferred_element_type=F32)


def mm_t(left, right):
    return lax.dot_general(left, right, (((0,), (0,)), ((), ())), preferred_element_type=F32)


def lanes(*parts):
    return jnp.concatenate(parts, axis=1)


def rows(*parts):
    return jnp.concatenate(parts, axis=0)


def iota2(axis):
    return lax.broadcasted_iota(jnp.int32, (C, C), axis)


def row_sum(x):
    return jnp.sum(x, axis=-1, keepdims=True)


def call(kernel, outs, ins, args, flops, scratch=()):
    size = sum(a.size * a.dtype.itemsize for a in args)
    return pl.pallas_call(
        kernel,
        out_shape=[jax.ShapeDtypeStruct(s, t) for s, t in outs],
        in_specs=ins,
        out_specs=[VMEM] * len(outs),
        scratch_shapes=list(scratch),
        cost_estimate=pl.CostEstimate(flops=flops, bytes_accessed=size, transcendentals=0),
    )(*args)


def masked_apply(left, wide, tall, keep):
    high, low = split2(left)
    both = mm(lanes(high, low), wide)
    inner = jnp.where(keep, both[:, :C], 0.0)
    s_high, s_low = split2(inner)
    return both[:, C:] + mm(lanes(s_high, s_low, high), tall)


def conjugate(rhs, apply_fn):
    count = len(rhs)
    each = range(count)
    sol = [None] * count
    res = list(rhs)
    sea = list(rhs)
    now = [row_sum(r * r) for r in res]
    for step in range(CG_STEPS):
        image = [apply_fn(c, sea[c]) for c in each]
        alpha = [now[c] / (row_sum(sea[c] * image[c]) + EPS) for c in each]
        sol = [alpha[c] * sea[c] if step == 0 else sol[c] + alpha[c] * sea[c] for c in each]
        if step == CG_STEPS - 1:
            break
        res = [res[c] - alpha[c] * image[c] for c in each]
        new = [row_sum(res[c] * res[c]) for c in each]
        sea = [res[c] + new[c] / (now[c] + EPS) * sea[c] for c in each]
        now = new
    return sol


def gram_kernel(k_ref, v_ref, out_ref):
    k = k_ref[...]
    both = mm_t(lanes(k, v_ref[...]), k)
    for j in range(XN):
        out_ref[j, :32] = both[32 * j : 32 * j + 32]
        out_ref[j, 32:] = both[D + 32 * j : D + 32 * j + 32]


def total_kernel(a_ref, out_ref):
    total = a_ref[0] + a_ref[1] + a_ref[2] + a_ref[3]
    for z in range(ZN):
        out_ref[z] = total


def before_kernel(z_ref, a_ref, b_ref, out_ref):
    z = z_ref[0]
    run = jnp.where(z > 0, b_ref[0], 0.0)
    for k in range(1, ZN - 1):
        run = run + jnp.where(k < z, b_ref[k], 0.0)
    for j in range(XN):
        out_ref[j] = run
        if j < XN - 1:
            run = run + a_ref[j]


def after_kernel(z_ref, a_ref, b_ref, out_ref, gain_ref):
    z = z_ref[0]
    run = jnp.where(z < ZN - 1, b_ref[ZN - 1, :64], 0.0)
    for k in range(1, ZN - 1):
        run = run + jnp.where(k > z, b_ref[k, :64], 0.0)
    for j in reversed(range(XN)):
        out_ref[j] = run
        if j > 0:
            run = run + a_ref[j, :64]
    gain = b_ref[0, 64:]
    for k in range(1, ZN):
        gain = gain + b_ref[k, 64:]
    gain_ref[...] = gain


def quarters(ref, start):
    return rows(*[ref[j, start : start + 32] for j in range(XN)])


def forward_kernel(ridge_ref, q_ref, k_ref, v_ref, g_ref, gain_ref, state_ref,
                   solved_ref, mixed_ref, sums_ref, wide_ref, tall_ref, assoc_ref):
    chunks = q_ref.shape[0] // C
    each = range(chunks)
    at = [slice(C * c, C * c + C) for c in each]
    keep = iota2(0) >= iota2(1)
    eye = iota2(0) == iota2(1)
    gram = quarters(state_ref, 0) + jnp.where(eye, ridge_ref[0], 0.0)
    assoc = quarters(state_ref, 32)
    turned = []
    for c in each:
        k = k_ref[at[c]]
        v = v_ref[at[c]]
        k_t = k.T
        turned.append(k_t)
        high, low = split2(gram)
        top = lanes(k_t, high)
        wide_ref[c, :C] = top
        wide_ref[c, C:] = top
        tall_ref[c] = rows(k, k, low)
        assoc_ref[c] = assoc
        if c < chunks - 1:
            more = mm(rows(k_t, v.T), k)
            gram = gram + more[:C]
            assoc = assoc + more[C:]
    solved = conjugate(
        [q_ref[at[c]].astype(F32) for c in each],
        lambda c, p: masked_apply(p, wide_ref[c], tall_ref[c], keep),
    )
    gain = gain_ref[...]
    ones = jnp.ones((8, 2 * D), BF16)
    for c in each:
        high, low = split2(assoc_ref[c].T)
        top = lanes(turned[c], high)
        v = v_ref[at[c]]
        mixed = masked_apply(solved[c], rows(top, top), rows(v, v, low), keep)
        solved_ref[at[c]] = solved[c]
        mixed_ref[at[c]] = mixed
        square = mixed * mixed
        cross = gain * g_ref[at[c]].astype(F32) * mixed
        for n, x in enumerate((square, cross)):
            total = lax.dot_general(
                ones, lanes(*split2(x)), (((1,), (1,)), ((), ())), preferred_element_type=F32
            )
            row = 4 * n + c
            for h in range(HEADS):
                sums_ref[h, row : row + 1] = total[:1]


def adjoint_kernel(k_ref, v_ref, g_ref, gain_ref, sums_ref, solved_ref, mixed_ref, wide_ref, tall_ref, assoc_ref,
                   out_ref, grad_q_ref, adjoint_ref, grad_mixed_ref, part_ref):
    chunks = k_ref.shape[0] // C
    each = range(chunks)
    at = [slice(C * c, C * c + C) for c in each]
    keep = iota2(0) >= iota2(1)
    gain = gain_ref[...]
    sums = sums_ref[0]
    for h in range(1, HEADS):
        sums = sums + sums_ref[h]
    columns = rows(sums, jnp.zeros((C - 8, C), F32)).T
    rhs = []
    gain_part = jnp.zeros((1, D), F32)
    grads = []
    for c in each:
        denom = jnp.sqrt(columns[:, c : c + 1] / (HEADS * D) + EPS)
        inverse = 1.0 / denom
        factor = columns[:, 4 + c : 5 + c] / (denom * denom * denom * (HEADS * D))
        mixed = mixed_ref[at[c]]
        scaled = mixed * inverse
        upstream = g_ref[at[c]].astype(F32)
        out_ref[at[c]] = (scaled * gain).astype(BF16)
        gain_part = gain_part + jnp.sum(upstream * scaled, axis=0, keepdims=True)
        grad = gain * upstream * inverse - mixed * factor
        grads.append(grad)
        grad_mixed_ref[at[c]] = grad
        k = k_ref[at[c]]
        high, low = split2(assoc_ref[c])
        top = lanes(v_ref[at[c]].T, high)
        rhs.append(masked_apply(grad, rows(top, top), rows(k, k, low), keep))
    adjoint = conjugate(rhs, lambda c, p: masked_apply(p, wide_ref[c], tall_ref[c], keep))
    total = None
    for c in each:
        adjoint_ref[at[c]] = adjoint[c]
        grad_q_ref[at[c]] = adjoint[c].astype(BF16)
        left_high, left_low = split2(rows(grads[c].T, adjoint[c].T))
        high, low = split2(solved_ref[at[c]])
        term = mm(lanes(left_high, left_low, left_high), rows(high, high, low))
        total = term if total is None else total + term
    suffix = total[:D]
    pairs = total[D:] + total[D:].T
    for j in range(XN):
        part_ref[j, :32] = suffix[32 * j : 32 * j + 32]
        part_ref[j, 32:64] = pairs[32 * j : 32 * j + 32]
        part_ref[j, 64:] = jnp.broadcast_to(gain_part, (8, D))


def local_kernel(k_ref, v_ref, solved_ref, adjoint_ref, grad_mixed_ref, grad_k_ref, grad_v_ref):
    chunks = k_ref.shape[0] // C
    keep = iota2(0) <= iota2(1)
    suffix = pairs = None
    for c in reversed(range(chunks)):
        at = slice(C * c, C * c + C)
        k = k_ref[at]
        v = v_ref[at]
        solved, adjoint, grad = solved_ref[at], adjoint_ref[at], grad_mixed_ref[at]
        s_high, s_low = split2(solved)
        a_high, a_low = split2(adjoint)
        g_high, g_low = split2(grad)
        st_high, st_low = split2(solved.T)
        at_high, at_low = split2(adjoint.T)
        gt_high, gt_low = split2(grad.T)
        both = mm(lanes(k, k), rows(lanes(st_high, at_high), lanes(st_low, at_low)))
        value_grad = mm(lanes(v, v), rows(gt_high, gt_low))
        key_solved = jnp.where(keep, both[:, :C], 0.0)
        other = jnp.where(keep, value_grad - both[:, C:], 0.0)
        ks_high, ks_low = split2(key_solved)
        o_high, o_low = split2(other)
        grad_v = mm(lanes(ks_high, ks_low, ks_high), rows(g_high, g_high, g_low))
        grad_k = mm(lanes(o_high, o_low, o_high), rows(s_high, s_high, s_low)) - mm(
            lanes(ks_high, ks_low, ks_high), rows(a_high, a_high, a_low)
        )
        if suffix is not None:
            more_k, more_v = finish(k, v, suffix, pairs)
            grad_k = grad_k + more_k
            grad_v = grad_v + more_v
        grad_k_ref[at] = grad_k
        grad_v_ref[at] = grad_v
        if c > 0:
            left_high, left_low = rows(gt_high, at_high), rows(gt_low, at_low)
            term = mm(lanes(left_high, left_low, left_high), rows(s_high, s_high, s_low))
            pair = term[D:] + term[D:].T
            suffix = term[:D] if suffix is None else suffix + term[:D]
            pairs = pair if pairs is None else pairs + pair


def finish(k, v, suffix, pairs):
    s_high, s_low = split2(suffix)
    p_high, p_low = split2(-pairs)
    t_high, t_low = split2(suffix.T)
    grad_k = mm(lanes(v, v), rows(s_high, s_low)) + mm(lanes(k, k), rows(p_high, p_low))
    return grad_k, mm(lanes(k, k), rows(t_high, t_low))


def last_kernel(k_ref, v_ref, state_ref, local_k_ref, local_v_ref, grad_k_ref, grad_v_ref):
    grad_k, grad_v = finish(k_ref[...], v_ref[...], quarters(state_ref, 0), quarters(state_ref, 32))
    grad_k_ref[...] = (local_k_ref[...] + grad_k).astype(BF16)
    grad_v_ref[...] = (local_v_ref[...] + grad_v).astype(BF16)


def exchange(array, axis):
    return lax.all_to_all(array, axis, split_axis=0, concat_axis=0, tiled=True)


def per_device(queries, keys, values, ridge, gain, grad_out):
    tok = queries.shape[0]
    chunks = tok // C
    z_index = lax.axis_index("z").reshape(1)
    gain_row = gain.reshape(1, D)
    token = (tok, D)

    (parts,) = call(gram_kernel, [((XN, 64, D), F32)], [VMEM] * 2, (keys, values), 4 * tok * D * D)
    parts = exchange(parts, "x")
    (copies,) = call(total_kernel, [((ZN, 64, D), F32)], [VMEM], (parts,), 10**5)
    copies = exchange(copies, "z")
    (state,) = call(before_kernel, [((XN, 64, D), F32)], [SMEM, VMEM, VMEM], (z_index, parts, copies), 10**5)
    state = exchange(state, "x")
    solved, mixed, sums, wide, tall, assoc = call(
        forward_kernel,
        [(token, F32), (token, F32), ((HEADS, 8, D), F32),
         ((chunks, 2 * C, 2 * D), BF16), ((chunks, 3 * C, D), BF16), ((chunks, D, D), F32)],
        [SMEM] + [VMEM] * 6,
        (ridge, queries, keys, values, grad_out, gain_row, state),
        10**9,
    )
    sums = exchange(sums, "head")
    output, grad_q, adjoint, grad_mixed, parts = call(
        adjoint_kernel,
        [(token, BF16), (token, BF16), (token, F32), (token, F32), ((XN, 72, D), F32)],
        [VMEM] * 10,
        (keys, values, grad_out, gain_row, sums, solved, mixed, wide, tall, assoc),
        10**9,
    )
    local_k, local_v = call(
        local_kernel,
        [(token, F32), (token, F32)],
        [VMEM] * 5,
        (keys, values, solved, adjoint, grad_mixed),
        5 * 10**8,
    )
    parts = exchange(parts, "x")
    (copies,) = call(total_kernel, [((ZN, 72, D), F32)], [VMEM], (parts,), 10**5)
    copies = exchange(copies, "z")
    state, grad_gain = call(
        after_kernel, [((XN, 64, D), F32), ((8, D), F32)], [SMEM, VMEM, VMEM], (z_index, parts, copies), 10**5
    )
    state = exchange(state, "x")
    grad_k, grad_v = call(
        last_kernel, [(token, BF16), (token, BF16)], [VMEM] * 5, (keys, values, state, local_k, local_v), 10**8
    )
    return output, grad_q, grad_k, grad_v, grad_gain[0]


def solution(mesh):
    split = Mesh(mesh.devices.reshape(ZN, XN, mesh.shape["head"]), ("z", "x", "head"))
    tokens = P(SEQ, "head")
    return jax.shard_map(
        per_device,
        mesh=split,
        in_specs=(tokens, tokens, tokens, P("head"), P("head"), tokens),
        out_specs=(tokens, tokens, tokens, tokens, P("head")),
        check_vma=False,
    )
```

```python
import jax
import jax.numpy as jnp
from jax import lax
from jax.experimental import pallas as pl
from jax.experimental.pallas import tpu as pltpu
from jax.sharding import Mesh
from jax.sharding import PartitionSpec as P

HEADS = 8
D = 128
CG_STEPS = 6
EPS = 1e-06
ZN = 8
XN = 4
SEQ = ("z", "x")
C = 128
F32 = jnp.float32
BF16 = jnp.bfloat16
VMEM = pl.BlockSpec(memory_space=pltpu.VMEM)
SMEM = pl.BlockSpec(memory_space=pltpu.SMEM)


def split2(x):
    high = x.astype(BF16)
    return high, (x - high.astype(F32)).astype(BF16)


def mm(left, right):
    return jnp.dot(left, right, preferred_element_type=F32)


def mm_t(left, right):
    return lax.dot_general(left, right, (((0,), (0,)), ((), ())), preferred_element_type=F32)


def lanes(*parts):
    return jnp.concatenate(parts, axis=1)


def rows(*parts):
    return jnp.concatenate(parts, axis=0)


def iota2(axis):
    return lax.broadcasted_iota(jnp.int32, (C, C), axis)


def row_sum(x):
    return jnp.sum(x, axis=-1, keepdims=True)


def call(kernel, outs, ins, args, flops, grant=8):
    size = sum(a.size * a.dtype.itemsize for a in args)
    return pl.pallas_call(
        kernel,
        out_shape=[jax.ShapeDtypeStruct(s, t) for s, t in outs],
        in_specs=ins,
        out_specs=[VMEM] * len(outs),
        compiler_params=pltpu.CompilerParams(vmem_limit_bytes=grant * 2**20),
        cost_estimate=pl.CostEstimate(flops=flops, bytes_accessed=size, transcendentals=0),
    )(*args)


def masked_apply(left, wide, tall, keep):
    high, low = split2(left)
    both = mm(lanes(high, low), wide)
    inner = jnp.where(keep, both[:, :C], 0.0)
    s_high, s_low = split2(inner)
    return both[:, C:] + mm(lanes(s_high, s_low, high), tall)


def conjugate(rhs, apply_fn):
    count = len(rhs)
    each = range(count)
    sol = [None] * count
    res = list(rhs)
    sea = list(rhs)
    now = [row_sum(r * r) for r in res]
    for step in range(CG_STEPS):
        image = [apply_fn(c, sea[c]) for c in each]
        alpha = [now[c] / (row_sum(sea[c] * image[c]) + EPS) for c in each]
        sol = [alpha[c] * sea[c] if step == 0 else sol[c] + alpha[c] * sea[c] for c in each]
        if step == CG_STEPS - 1:
            break
        res = [res[c] - alpha[c] * image[c] for c in each]
        new = [row_sum(res[c] * res[c]) for c in each]
        sea = [res[c] + new[c] / (now[c] + EPS) * sea[c] for c in each]
        now = new
    return sol


def gram_kernel(k_ref, v_ref, out_ref):
    k = k_ref[...]
    both = mm_t(lanes(k, v_ref[...]), k)
    for j in range(XN):
        out_ref[j, :32] = both[32 * j : 32 * j + 32]
        out_ref[j, 32:] = both[D + 32 * j : D + 32 * j + 32]


def total_kernel(a_ref, out_ref):
    total = a_ref[0] + a_ref[1] + a_ref[2] + a_ref[3]
    for z in range(ZN):
        out_ref[z] = total


def before_kernel(z_ref, a_ref, b_ref, out_ref):
    z = z_ref[0]
    run = jnp.where(z > 0, b_ref[0], 0.0)
    for k in range(1, ZN - 1):
        run = run + jnp.where(k < z, b_ref[k], 0.0)
    for j in range(XN):
        out_ref[j] = run
        if j < XN - 1:
            run = run + a_ref[j]


def after_kernel(z_ref, a_ref, b_ref, out_ref, gain_ref):
    z = z_ref[0]
    run = jnp.where(z < ZN - 1, b_ref[ZN - 1, :64], 0.0)
    for k in range(1, ZN - 1):
        run = run + jnp.where(k > z, b_ref[k, :64], 0.0)
    for j in reversed(range(XN)):
        out_ref[j] = run
        if j > 0:
            run = run + a_ref[j, :64]
    gain = b_ref[0, 64:]
    for k in range(1, ZN):
        gain = gain + b_ref[k, 64:]
    gain_ref[...] = gain


def quarters(ref, start):
    return rows(*[ref[j, start : start + 32] for j in range(XN)])


def forward_kernel(ridge_ref, q_ref, k_ref, v_ref, g_ref, gain_ref, state_ref,
                   solved_ref, mixed_ref, sums_ref, wide_ref, tall_ref, assoc_ref):
    chunks = q_ref.shape[0] // C
    each = range(chunks)
    at = [slice(C * c, C * c + C) for c in each]
    keep = iota2(0) >= iota2(1)
    eye = iota2(0) == iota2(1)
    gram = quarters(state_ref, 0) + jnp.where(eye, ridge_ref[0], 0.0)
    assoc = quarters(state_ref, 32)
    turned = []
    for c in each:
        k = k_ref[at[c]]
        v = v_ref[at[c]]
        k_t = k.T
        turned.append(k_t)
        high, low = split2(gram)
        top = lanes(k_t, high)
        wide_ref[c, :C] = top
        wide_ref[c, C:] = top
        tall_ref[c] = rows(k, k, low)
        assoc_ref[c] = assoc
        if c < chunks - 1:
            more = mm(rows(k_t, v.T), k)
            gram = gram + more[:C]
            assoc = assoc + more[C:]
    solved = conjugate(
        [q_ref[at[c]].astype(F32) for c in each],
        lambda c, p: masked_apply(p, wide_ref[c], tall_ref[c], keep),
    )
    gain = gain_ref[...]
    ones = jnp.ones((8, 2 * D), BF16)
    for c in each:
        high, low = split2(assoc_ref[c].T)
        top = lanes(turned[c], high)
        v = v_ref[at[c]]
        mixed = masked_apply(solved[c], rows(top, top), rows(v, v, low), keep)
        solved_ref[at[c]] = solved[c]
        mixed_ref[at[c]] = mixed
        square = mixed * mixed
        cross = gain * g_ref[at[c]].astype(F32) * mixed
        for n, x in enumerate((square, cross)):
            total = lax.dot_general(
                ones, lanes(*split2(x)), (((1,), (1,)), ((), ())), preferred_element_type=F32
            )
            row = 4 * n + c
            for h in range(HEADS):
                sums_ref[h, row : row + 1] = total[:1]


def adjoint_kernel(k_ref, v_ref, g_ref, gain_ref, sums_ref, solved_ref, mixed_ref, wide_ref, tall_ref, assoc_ref,
                   out_ref, grad_q_ref, adjoint_ref, grad_mixed_ref, part_ref):
    chunks = k_ref.shape[0] // C
    each = range(chunks)
    at = [slice(C * c, C * c + C) for c in each]
    keep = iota2(0) >= iota2(1)
    gain = gain_ref[...]
    sums = sums_ref[0]
    for h in range(1, HEADS):
        sums = sums + sums_ref[h]
    columns = rows(sums, jnp.zeros((C - 8, C), F32)).T
    rhs = []
    gain_part = jnp.zeros((1, D), F32)
    grads = []
    for c in each:
        denom = jnp.sqrt(columns[:, c : c + 1] / (HEADS * D) + EPS)
        inverse = 1.0 / denom
        factor = columns[:, 4 + c : 5 + c] / (denom * denom * denom * (HEADS * D))
        mixed = mixed_ref[at[c]]
        scaled = mixed * inverse
        upstream = g_ref[at[c]].astype(F32)
        out_ref[at[c]] = (scaled * gain).astype(BF16)
        gain_part = gain_part + jnp.sum(upstream * scaled, axis=0, keepdims=True)
        grad = gain * upstream * inverse - mixed * factor
        grads.append(grad)
        grad_mixed_ref[at[c]] = grad
        k = k_ref[at[c]]
        high, low = split2(assoc_ref[c])
        top = lanes(v_ref[at[c]].T, high)
        rhs.append(masked_apply(grad, rows(top, top), rows(k, k, low), keep))
    adjoint = conjugate(rhs, lambda c, p: masked_apply(p, wide_ref[c], tall_ref[c], keep))
    total = None
    for c in each:
        adjoint_ref[at[c]] = adjoint[c]
        grad_q_ref[at[c]] = adjoint[c].astype(BF16)
        left_high, left_low = split2(rows(grads[c].T, adjoint[c].T))
        high, low = split2(solved_ref[at[c]])
        term = mm(lanes(left_high, left_low, left_high), rows(high, high, low))
        total = term if total is None else total + term
    suffix = total[:D]
    pairs = total[D:] + total[D:].T
    for j in range(XN):
        part_ref[j, :32] = suffix[32 * j : 32 * j + 32]
        part_ref[j, 32:64] = pairs[32 * j : 32 * j + 32]
        part_ref[j, 64:] = jnp.broadcast_to(gain_part, (8, D))


def local_kernel(k_ref, v_ref, solved_ref, adjoint_ref, grad_mixed_ref, grad_k_ref, grad_v_ref):
    chunks = k_ref.shape[0] // C
    keep = iota2(0) <= iota2(1)
    suffix = pairs = None
    for c in reversed(range(chunks)):
        at = slice(C * c, C * c + C)
        k = k_ref[at]
        v = v_ref[at]
        solved, adjoint, grad = solved_ref[at], adjoint_ref[at], grad_mixed_ref[at]
        s_high, s_low = split2(solved)
        a_high, a_low = split2(adjoint)
        g_high, g_low = split2(grad)
        st_high, st_low = split2(solved.T)
        at_high, at_low = split2(adjoint.T)
        gt_high, gt_low = split2(grad.T)
        both = mm(lanes(k, k), rows(lanes(st_high, at_high), lanes(st_low, at_low)))
        value_grad = mm(lanes(v, v), rows(gt_high, gt_low))
        key_solved = jnp.where(keep, both[:, :C], 0.0)
        other = jnp.where(keep, value_grad - both[:, C:], 0.0)
        ks_high, ks_low = split2(key_solved)
        o_high, o_low = split2(other)
        grad_v = mm(lanes(ks_high, ks_low, ks_high), rows(g_high, g_high, g_low))
        grad_k = mm(lanes(o_high, o_low, o_high), rows(s_high, s_high, s_low)) - mm(
            lanes(ks_high, ks_low, ks_high), rows(a_high, a_high, a_low)
        )
        if suffix is not None:
            more_k, more_v = finish(k, v, suffix, pairs)
            grad_k = grad_k + more_k
            grad_v = grad_v + more_v
        grad_k_ref[at] = grad_k
        grad_v_ref[at] = grad_v
        if c > 0:
            left_high, left_low = rows(gt_high, at_high), rows(gt_low, at_low)
            term = mm(lanes(left_high, left_low, left_high), rows(s_high, s_high, s_low))
            pair = term[D:] + term[D:].T
            suffix = term[:D] if suffix is None else suffix + term[:D]
            pairs = pair if pairs is None else pairs + pair


def finish(k, v, suffix, pairs):
    s_high, s_low = split2(suffix)
    p_high, p_low = split2(-pairs)
    t_high, t_low = split2(suffix.T)
    grad_k = mm(lanes(v, v), rows(s_high, s_low)) + mm(lanes(k, k), rows(p_high, p_low))
    return grad_k, mm(lanes(k, k), rows(t_high, t_low))


def last_kernel(k_ref, v_ref, state_ref, local_k_ref, local_v_ref, grad_k_ref, grad_v_ref):
    grad_k, grad_v = finish(k_ref[...], v_ref[...], quarters(state_ref, 0), quarters(state_ref, 32))
    grad_k_ref[...] = (local_k_ref[...] + grad_k).astype(BF16)
    grad_v_ref[...] = (local_v_ref[...] + grad_v).astype(BF16)


def exchange(array, axis):
    return lax.all_to_all(array, axis, split_axis=0, concat_axis=0, tiled=True)


def per_device(queries, keys, values, ridge, gain, grad_out):
    tok = queries.shape[0]
    chunks = tok // C
    z_index = lax.axis_index("z").reshape(1)
    gain_row = gain.reshape(1, D)
    token = (tok, D)

    (parts,) = call(gram_kernel, [((XN, 64, D), F32)], [VMEM] * 2, (keys, values), 4 * tok * D * D)
    parts = exchange(parts, "x")
    (copies,) = call(total_kernel, [((ZN, 64, D), F32)], [VMEM], (parts,), 10**5)
    copies = exchange(copies, "z")
    (state,) = call(before_kernel, [((XN, 64, D), F32)], [SMEM, VMEM, VMEM], (z_index, parts, copies), 10**5)
    state = exchange(state, "x")
    solved, mixed, sums, wide, tall, assoc = call(
        forward_kernel,
        [(token, F32), (token, F32), ((HEADS, 8, D), F32),
         ((chunks, 2 * C, 2 * D), BF16), ((chunks, 3 * C, D), BF16), ((chunks, D, D), F32)],
        [SMEM] + [VMEM] * 6,
        (ridge, queries, keys, values, grad_out, gain_row, state),
        10**9,
    )
    sums = exchange(sums, "head")
    output, grad_q, adjoint, grad_mixed, parts = call(
        adjoint_kernel,
        [(token, BF16), (token, BF16), (token, F32), (token, F32), ((XN, 72, D), F32)],
        [VMEM] * 10,
        (keys, values, grad_out, gain_row, sums, solved, mixed, wide, tall, assoc),
        10**9,
    )
    local_k, local_v = call(
        local_kernel,
        [(token, F32), (token, F32)],
        [VMEM] * 5,
        (keys, values, solved, adjoint, grad_mixed),
        5 * 10**8,
    )
    parts = exchange(parts, "x")
    (copies,) = call(total_kernel, [((ZN, 72, D), F32)], [VMEM], (parts,), 10**5)
    copies = exchange(copies, "z")
    state, grad_gain = call(
        after_kernel, [((XN, 64, D), F32), ((8, D), F32)], [SMEM, VMEM, VMEM], (z_index, parts, copies), 10**5
    )
    state = exchange(state, "x")
    grad_k, grad_v = call(
        last_kernel, [(token, BF16), (token, BF16)], [VMEM] * 5, (keys, values, state, local_k, local_v), 10**8
    )
    return output, grad_q, grad_k, grad_v, grad_gain[0]


def solution(mesh):
    split = Mesh(mesh.devices.reshape(ZN, XN, mesh.shape["head"]), ("z", "x", "head"))
    tokens = P(SEQ, "head")
    return jax.shard_map(
        per_device,
        mesh=split,
        in_specs=(tokens, tokens, tokens, P("head"), P("head"), tokens),
        out_specs=(tokens, tokens, tokens, tokens, P("head")),
        check_vma=False,
    )
```

```python
import jax
import jax.numpy as jnp
from jax import lax
from jax.experimental import pallas as pl
from jax.experimental.pallas import tpu as pltpu
from jax.sharding import Mesh
from jax.sharding import PartitionSpec as P

HEADS = 8
D = 128
CG_STEPS = 6
EPS = 1e-06
ZN = 8
XN = 4
SLICES = ZN * XN
GAIN_SLICE = 25
SEQ = ("z", "x")
C = 128
F32 = jnp.float32
BF16 = jnp.bfloat16
VMEM = pl.BlockSpec(memory_space=pltpu.VMEM)
HBM = pl.BlockSpec(memory_space=pltpu.HBM)


def split2(x):
    high = x.astype(BF16)
    return high, (x - high.astype(F32)).astype(BF16)


def mm(left, right):
    return jnp.dot(left, right, preferred_element_type=F32)


def mm_t(left, right):
    return lax.dot_general(left, right, (((0,), (0,)), ((), ())), preferred_element_type=F32)


def lanes(*parts):
    return jnp.concatenate(parts, axis=1)


def rows(*parts):
    return jnp.concatenate(parts, axis=0)


def iota2(axis):
    return lax.broadcasted_iota(jnp.int32, (C, C), axis)


def row_sum(x):
    return jnp.sum(x, axis=-1, keepdims=True)


def call(kernel, outs, ins, args, flops, grant=8192, scratch=()):
    size = sum(a.size * a.dtype.itemsize for a in args)
    return pl.pallas_call(
        kernel,
        out_shape=[jax.ShapeDtypeStruct(s, t) for s, t in outs],
        in_specs=ins,
        out_specs=[VMEM] * len(outs),
        scratch_shapes=list(scratch),
        compiler_params=pltpu.CompilerParams(vmem_limit_bytes=grant * 2**10),
        cost_estimate=pl.CostEstimate(flops=flops, bytes_accessed=size, transcendentals=0),
    )(*args)


def masked_apply(left, wide, tall, keep):
    high, low = split2(left)
    both = mm(lanes(high, low), wide)
    inner = jnp.where(keep, both[:, :C], 0.0)
    s_high, s_low = split2(inner)
    return both[:, C:] + mm(lanes(s_high, s_low, high), tall)


def conjugate(rhs, apply_fn):
    count = len(rhs)
    each = range(count)
    sol = [None] * count
    res = list(rhs)
    sea = list(rhs)
    now = [row_sum(r * r) for r in res]
    for step in range(CG_STEPS):
        image = [apply_fn(c, sea[c]) for c in each]
        alpha = [now[c] / (row_sum(sea[c] * image[c]) + EPS) for c in each]
        sol = [alpha[c] * sea[c] if step == 0 else sol[c] + alpha[c] * sea[c] for c in each]
        if step == CG_STEPS - 1:
            break
        res = [res[c] - alpha[c] * image[c] for c in each]
        new = [row_sum(res[c] * res[c]) for c in each]
        sea = [res[c] + new[c] / (now[c] + EPS) * sea[c] for c in each]
        now = new
    return sol


def gram_kernel(k_hbm, v_hbm, out_ref, k_ref, v_ref, sem):
    copies = [
        pltpu.make_async_copy(k_hbm, k_ref, sem.at[0]),
        pltpu.make_async_copy(v_hbm, v_ref, sem.at[1]),
    ]
    for copy in copies:
        copy.start()
    for copy in copies:
        copy.wait()
    k = k_ref[...]
    out_ref[...] = mm_t(lanes(k, v_ref[...]), k)


def before_kernel(a_ref, out_ref):
    run = jnp.zeros((8, D), F32)
    for k in range(SLICES):
        out_ref[k] = run
        run = run + a_ref[k]


def after_kernel(a_ref, out_ref):
    total = a_ref[0]
    for k in range(1, SLICES):
        total = total + a_ref[k]
    whole = lax.axis_index("z") * XN + lax.axis_index("x") == GAIN_SLICE
    run = jnp.zeros((8, D), F32)
    for k in reversed(range(SLICES)):
        out_ref[k] = jnp.where(whole, total, run)
        run = run + a_ref[k]


def pack(pairs):
    row = lax.broadcasted_iota(jnp.int32, (C // 2, C), 0)
    col = lax.broadcasted_iota(jnp.int32, (C // 2, C), 1)
    turned = pltpu.roll(pairs[C // 2 :], C // 2, 1)
    return jnp.where((col < C // 2) & (col > row), turned, pairs[: C // 2])


def unpack(packed, diagonal):
    row, col = iota2(0), iota2(1)
    half = C // 2
    both = rows(packed, pltpu.roll(packed, half, 1))
    direct = ((row < half) & ((col >= half) | (row >= col))) | ((row >= half) & (col >= half) & (row < col))
    return jnp.where(row == col, diagonal, jnp.where(direct, both, both.T))


def forward_kernel(ridge_ref, q_ref, k_ref, v_ref, g_ref, gain_ref, state_ref,
                   solved_ref, mixed_ref, sums_ref, wide_ref, tall_ref, assoc_ref):
    chunks = q_ref.shape[0] // C
    each = range(chunks)
    at = [slice(C * c, C * c + C) for c in each]
    keep = iota2(0) >= iota2(1)
    eye = iota2(0) == iota2(1)
    gram = state_ref[:D] + jnp.where(eye, ridge_ref[...], 0.0)
    assoc = state_ref[D:]
    turned = []
    for c in each:
        k = k_ref[at[c]]
        v = v_ref[at[c]]
        k_t = k.T
        turned.append(k_t)
        high, low = split2(gram)
        top = lanes(k_t, high)
        wide_ref[c, :C] = top
        wide_ref[c, C:] = top
        tall_ref[c] = rows(k, k, low)
        assoc_ref[c] = assoc
        if c < chunks - 1:
            more = mm(rows(k_t, v.T), k)
            gram = gram + more[:C]
            assoc = assoc + more[C:]
    solved = conjugate(
        [q_ref[at[c]].astype(F32) for c in each],
        lambda c, p: masked_apply(p, wide_ref[c], tall_ref[c], keep),
    )
    gain = gain_ref[...]
    ones = jnp.ones((8, 2 * D), BF16)
    for c in each:
        high, low = split2(assoc_ref[c].T)
        top = lanes(turned[c], high)
        v = v_ref[at[c]]
        mixed = masked_apply(solved[c], rows(top, top), rows(v, v, low), keep)
        solved_ref[at[c]] = solved[c]
        mixed_ref[at[c]] = mixed
        square = mixed * mixed
        cross = gain * g_ref[at[c]].astype(F32) * mixed
        for n, x in enumerate((square, cross)):
            total = lax.dot_general(
                ones, lanes(*split2(x)), (((1,), (1,)), ((), ())), preferred_element_type=F32
            )
            row = 4 * n + c
            for h in range(HEADS):
                sums_ref[h, row : row + 1] = total[:1]


def adjoint_kernel(k_ref, v_ref, g_ref, gain_ref, sums_ref, solved_ref, mixed_ref, wide_ref, tall_ref, assoc_ref,
                   out_ref, grad_q_ref, adjoint_ref, grad_mixed_ref, part_ref):
    chunks = k_ref.shape[0] // C
    each = range(chunks)
    at = [slice(C * c, C * c + C) for c in each]
    keep = iota2(0) >= iota2(1)
    gain = gain_ref[...]
    sums = sums_ref[0]
    for h in range(1, HEADS):
        sums = sums + sums_ref[h]
    columns = rows(sums, jnp.zeros((C - 8, C), F32)).T
    rhs = []
    gain_part = jnp.zeros((8, D), F32)
    grads = []
    for c in each:
        denom = jnp.sqrt(columns[:, c : c + 1] / (HEADS * D) + EPS)
        inverse = 1.0 / denom
        factor = columns[:, 4 + c : 5 + c] / (denom * denom * denom * (HEADS * D))
        mixed = mixed_ref[at[c]]
        scaled = mixed * inverse
        upstream = g_ref[at[c]].astype(F32)
        out_ref[at[c]] = (scaled * gain).astype(BF16)
        gain_part = gain_part + jnp.sum((upstream * scaled).reshape(C // 8, 8, D), axis=0)
        grad = gain * upstream * inverse - mixed * factor
        grads.append(grad)
        grad_mixed_ref[at[c]] = grad
        k = k_ref[at[c]]
        high, low = split2(assoc_ref[c])
        top = lanes(v_ref[at[c]].T, high)
        rhs.append(masked_apply(grad, rows(top, top), rows(k, k, low), keep))
    adjoint = conjugate(rhs, lambda c, p: masked_apply(p, wide_ref[c], tall_ref[c], keep))
    total = None
    for c in each:
        adjoint_ref[at[c]] = adjoint[c]
        grad_q_ref[at[c]] = adjoint[c].astype(BF16)
        left_high, left_low = split2(rows(grads[c].T, adjoint[c].T))
        high, low = split2(solved_ref[at[c]])
        term = mm(lanes(left_high, left_low, left_high), rows(high, high, low))
        total = term if total is None else total + term
    pairs = total[D:] + total[D:].T
    part_ref[:D] = total[:D]
    part_ref[D : D + 64] = pack(pairs)
    diagonal = jnp.sum(jnp.where(iota2(0) == iota2(1), pairs, 0.0), axis=0, keepdims=True)
    part_ref[D + 64 : D + 72] = jnp.broadcast_to(diagonal, (8, D))
    part_ref[D + 72 : D + 80] = gain_part
    part_ref[D + 80 :] = jnp.zeros((D - 80, D), F32)


def local_kernel(k_ref, v_ref, solved_ref, adjoint_ref, grad_mixed_ref, grad_k_ref, grad_v_ref):
    chunks = k_ref.shape[0] // C
    keep = iota2(0) <= iota2(1)
    suffix = pairs = None
    for c in reversed(range(chunks)):
        at = slice(C * c, C * c + C)
        k = k_ref[at]
        v = v_ref[at]
        solved, adjoint, grad = solved_ref[at], adjoint_ref[at], grad_mixed_ref[at]
        s_high, s_low = split2(solved)
        a_high, a_low = split2(adjoint)
        g_high, g_low = split2(grad)
        st_high, st_low = split2(solved.T)
        at_high, at_low = split2(adjoint.T)
        gt_high, gt_low = split2(grad.T)
        both = mm(lanes(k, k), rows(lanes(st_high, at_high), lanes(st_low, at_low)))
        value_grad = mm(lanes(v, v), rows(gt_high, gt_low))
        key_solved = jnp.where(keep, both[:, :C], 0.0)
        other = jnp.where(keep, value_grad - both[:, C:], 0.0)
        ks_high, ks_low = split2(key_solved)
        o_high, o_low = split2(other)
        grad_v = mm(lanes(ks_high, ks_low, ks_high), rows(g_high, g_high, g_low))
        grad_k = mm(lanes(o_high, o_low, o_high), rows(s_high, s_high, s_low)) - mm(
            lanes(ks_high, ks_low, ks_high), rows(a_high, a_high, a_low)
        )
        if suffix is not None:
            more_k, more_v = finish(k, v, suffix, pairs)
            grad_k = grad_k + more_k
            grad_v = grad_v + more_v
        grad_k_ref[at] = grad_k
        grad_v_ref[at] = grad_v
        if c > 0:
            left_high, left_low = rows(gt_high, at_high), rows(gt_low, at_low)
            term = mm(lanes(left_high, left_low, left_high), rows(s_high, s_high, s_low))
            pair = term[D:] + term[D:].T
            suffix = term[:D] if suffix is None else suffix + term[:D]
            pairs = pair if pairs is None else pairs + pair


def finish(k, v, suffix, pairs):
    s_high, s_low = split2(suffix)
    p_high, p_low = split2(-pairs)
    t_high, t_low = split2(suffix.T)
    grad_k = mm(lanes(v, v), rows(s_high, s_low)) + mm(lanes(k, k), rows(p_high, p_low))
    return grad_k, mm(lanes(k, k), rows(t_high, t_low))


def last_kernel(k_ref, v_ref, state_ref, local_k_ref, local_v_ref, grad_k_ref, grad_v_ref, gain_ref):
    pairs = unpack(state_ref[D : D + 64], state_ref[D + 64 : D + 65])
    grad_k, grad_v = finish(k_ref[...], v_ref[...], state_ref[:D], pairs)
    grad_k_ref[...] = (local_k_ref[...] + grad_k).astype(BF16)
    grad_v_ref[...] = (local_v_ref[...] + grad_v).astype(BF16)
    gain_ref[...] = jnp.sum(state_ref[D + 72 : D + 80], axis=0, keepdims=True)


def exchange(array, axis):
    return lax.all_to_all(array, axis, split_axis=0, concat_axis=0, tiled=True)


def scan_over_seq(kernel, parts):
    slices = (SLICES, 8, D)
    held = exchange(parts.reshape(slices), SEQ)
    (held,) = call(kernel, [(slices, F32)], [VMEM], (held,), 10**5)
    return exchange(held, SEQ).reshape(2 * D, D)


def per_device(queries, keys, values, ridge, gain, grad_out):
    tok = queries.shape[0]
    chunks = tok // C
    gain_row = gain.reshape(1, D)
    token = (tok, D)
    state_shape = ((2 * D, D), F32)

    (parts,) = call(
        gram_kernel, [state_shape], [HBM] * 2, (keys, values), 4 * tok * D * D, grant=55000,
        scratch=[pltpu.VMEM(token, BF16), pltpu.VMEM(token, BF16), pltpu.SemaphoreType.DMA((2,))],
    )
    ridge_row = jnp.broadcast_to(ridge.reshape(1, 1), (1, D))
    parts, ridge_row = lax.optimization_barrier((parts, ridge_row))
    state = scan_over_seq(before_kernel, parts)
    solved, mixed, sums, wide, tall, assoc = call(
        forward_kernel,
        [(token, F32), (token, F32), ((HEADS, 8, D), F32),
         ((chunks, 2 * C, 2 * D), BF16), ((chunks, 3 * C, D), BF16), ((chunks, D, D), F32)],
        [VMEM] * 7,
        (ridge_row, queries, keys, values, grad_out, gain_row, state),
        10**9,
    )
    sums = exchange(sums, "head")
    output, grad_q, adjoint, grad_mixed, parts = call(
        adjoint_kernel,
        [(token, BF16), (token, BF16), (token, F32), (token, F32), state_shape],
        [VMEM] * 10,
        (keys, values, grad_out, gain_row, sums, solved, mixed, wide, tall, assoc),
        10**9,
    )
    local_k, local_v = call(
        local_kernel,
        [(token, F32), (token, F32)],
        [VMEM] * 5,
        (keys, values, solved, adjoint, grad_mixed),
        5 * 10**8,
    )
    state = scan_over_seq(after_kernel, parts)
    grad_k, grad_v, grad_gain = call(
        last_kernel, [(token, BF16), (token, BF16), ((1, D), F32)], [VMEM] * 5,
        (keys, values, state, local_k, local_v), 10**8,
    )
    return output, grad_q, grad_k, grad_v, grad_gain.reshape(D)


def solution(mesh):
    split = Mesh(mesh.devices.reshape(ZN, XN, mesh.shape["head"]), ("z", "x", "head"))
    tokens = P(SEQ, "head")
    return jax.shard_map(
        per_device,
        mesh=split,
        in_specs=(tokens, tokens, tokens, P("head"), P("head"), tokens),
        out_specs=(tokens, tokens, tokens, tokens, P("head")),
        check_vma=False,
    )
```

```python
import jax
import jax.numpy as jnp
from jax import lax
from jax.experimental import pallas as pl
from jax.experimental.pallas import tpu as pltpu
from jax.sharding import Mesh
from jax.sharding import PartitionSpec as P

HEADS = 8
D = 128
CG_STEPS = 6
EPS = 1e-06
ZN = 8
XN = 4
SLICES = ZN * XN
GAIN_SLICE = 25
SEQ = ("z", "x")
C = 128
F32 = jnp.float32
BF16 = jnp.bfloat16
VMEM = pl.BlockSpec(memory_space=pltpu.VMEM)
HBM = pl.BlockSpec(memory_space=pltpu.HBM)


def split2(x):
    high = x.astype(BF16)
    return high, (x - high.astype(F32)).astype(BF16)


def mm(left, right):
    return jnp.dot(left, right, preferred_element_type=F32)


def mm_t(left, right):
    return lax.dot_general(left, right, (((0,), (0,)), ((), ())), preferred_element_type=F32)


def lanes(*parts):
    return jnp.concatenate(parts, axis=1)


def rows(*parts):
    return jnp.concatenate(parts, axis=0)


def iota2(axis):
    return lax.broadcasted_iota(jnp.int32, (C, C), axis)


def row_sum(x):
    return jnp.sum(x, axis=-1, keepdims=True)


def call(kernel, outs, ins, args, flops, grant=8192, scratch=(), places=None):
    size = sum(a.size * a.dtype.itemsize for a in args)
    return pl.pallas_call(
        kernel,
        out_shape=[jax.ShapeDtypeStruct(s, t) for s, t in outs],
        in_specs=ins,
        out_specs=places or [VMEM] * len(outs),
        scratch_shapes=list(scratch),
        compiler_params=pltpu.CompilerParams(vmem_limit_bytes=grant * 2**10),
        cost_estimate=pl.CostEstimate(flops=flops, bytes_accessed=size, transcendentals=0),
    )(*args)


def masked_apply(left, wide, tall, keep):
    high, low = split2(left)
    both = mm(lanes(high, low), wide)
    inner = jnp.where(keep, both[:, :C], 0.0)
    s_high, s_low = split2(inner)
    return both[:, C:] + mm(lanes(s_high, s_low, high), tall)


def conjugate(rhs, apply_fn):
    count = len(rhs)
    each = range(count)
    sol = [None] * count
    res = list(rhs)
    sea = list(rhs)
    now = [row_sum(r * r) for r in res]
    for step in range(CG_STEPS):
        image = [apply_fn(c, sea[c]) for c in each]
        alpha = [now[c] / (row_sum(sea[c] * image[c]) + EPS) for c in each]
        sol = [alpha[c] * sea[c] if step == 0 else sol[c] + alpha[c] * sea[c] for c in each]
        if step == CG_STEPS - 1:
            break
        res = [res[c] - alpha[c] * image[c] for c in each]
        new = [row_sum(res[c] * res[c]) for c in each]
        sea = [res[c] + new[c] / (now[c] + EPS) * sea[c] for c in each]
        now = new
    return sol


def gram_kernel(k_hbm, v_hbm, out_ref, k_ref, v_ref, sem):
    half = k_hbm.shape[0] // 2
    at = [pl.ds(half * n, half) for n in range(2)]
    copies = [
        pltpu.make_async_copy(source.at[at[n]], target.at[at[n]], sem.at[n, m])
        for n in range(2)
        for m, (source, target) in enumerate(((k_hbm, k_ref), (v_hbm, v_ref)))
    ]
    for copy in copies:
        copy.start()
    total = None
    for n in range(2):
        copies[2 * n].wait()
        copies[2 * n + 1].wait()
        k = k_ref[at[n]]
        term = mm_t(lanes(k, v_ref[at[n]]), k)
        total = term if total is None else total + term
    out_ref[...] = total


def before_kernel(a_ref, out_ref):
    run = jnp.zeros((8, D), F32)
    for k in range(SLICES):
        out_ref[k] = run
        run = run + a_ref[k]


def after_kernel(a_ref, out_ref):
    total = a_ref[0]
    for k in range(1, SLICES):
        total = total + a_ref[k]
    whole = lax.axis_index("z") * XN + lax.axis_index("x") == GAIN_SLICE
    run = jnp.zeros((8, D), F32)
    for k in reversed(range(SLICES)):
        out_ref[k] = jnp.where(whole, total, run)
        run = run + a_ref[k]


def pack(pairs):
    row = lax.broadcasted_iota(jnp.int32, (C // 2, C), 0)
    col = lax.broadcasted_iota(jnp.int32, (C // 2, C), 1)
    turned = pltpu.roll(pairs[C // 2 :], C // 2, 1)
    return jnp.where((col < C // 2) & (col > row), turned, pairs[: C // 2])


def unpack(packed, diagonal):
    row, col = iota2(0), iota2(1)
    half = C // 2
    both = rows(packed, pltpu.roll(packed, half, 1))
    direct = ((row < half) & ((col >= half) | (row >= col))) | ((row >= half) & (col >= half) & (row < col))
    return jnp.where(row == col, diagonal, jnp.where(direct, both, both.T))


def forward_kernel(ridge_ref, gain_ref, q_ref, k_ref, v_ref, g_ref, state_ref,
                   solved_ref, mixed_ref, sums_ref, wide_ref, tall_ref, assoc_ref):
    chunks = q_ref.shape[0] // C
    each = range(chunks)
    at = [slice(C * c, C * c + C) for c in each]
    keep = iota2(0) >= iota2(1)
    eye = iota2(0) == iota2(1)
    gram = state_ref[:D] + jnp.where(eye, ridge_ref[...], 0.0)
    assoc = state_ref[D:]
    turned = []
    for c in each:
        k = k_ref[at[c]]
        v = v_ref[at[c]]
        k_t = k.T
        turned.append(k_t)
        high, low = split2(gram)
        top = lanes(k_t, high)
        wide_ref[c, :C] = top
        wide_ref[c, C:] = top
        tall_ref[c] = rows(k, k, low)
        assoc_ref[c] = assoc
        if c < chunks - 1:
            more = mm(rows(k_t, v.T), k)
            gram = gram + more[:C]
            assoc = assoc + more[C:]
    solved = conjugate(
        [q_ref[at[c]].astype(F32) for c in each],
        lambda c, p: masked_apply(p, wide_ref[c], tall_ref[c], keep),
    )
    gain = gain_ref[...]
    ones = jnp.ones((8, 2 * D), BF16)
    for c in each:
        high, low = split2(assoc_ref[c].T)
        top = lanes(turned[c], high)
        v = v_ref[at[c]]
        mixed = masked_apply(solved[c], rows(top, top), rows(v, v, low), keep)
        solved_ref[at[c]] = solved[c]
        mixed_ref[at[c]] = mixed
        square = mixed * mixed
        cross = gain * g_ref[at[c]].astype(F32) * mixed
        for n, x in enumerate((square, cross)):
            total = lax.dot_general(
                ones, lanes(*split2(x)), (((1,), (1,)), ((), ())), preferred_element_type=F32
            )
            row = 4 * n + c
            for h in range(HEADS):
                sums_ref[h, row : row + 1] = total[:1]


def adjoint_kernel(gain_ref, k_ref, v_ref, g_ref, sums_ref, solved_ref, mixed_ref, wide_ref, tall_ref, assoc_ref,
                   out_ref, adjoint_ref, grad_mixed_ref, part_ref):
    chunks = k_ref.shape[0] // C
    each = range(chunks)
    at = [slice(C * c, C * c + C) for c in each]
    keep = iota2(0) >= iota2(1)
    gain = gain_ref[...]
    sums = sums_ref[0]
    for h in range(1, HEADS):
        sums = sums + sums_ref[h]
    columns = rows(sums, jnp.zeros((C - 8, C), F32)).T
    rhs = []
    gain_part = jnp.zeros((8, D), F32)
    grads = []
    for c in each:
        denom = jnp.sqrt(columns[:, c : c + 1] / (HEADS * D) + EPS)
        inverse = 1.0 / denom
        factor = columns[:, 4 + c : 5 + c] / (denom * denom * denom * (HEADS * D))
        mixed = mixed_ref[at[c]]
        scaled = mixed * inverse
        upstream = g_ref[at[c]].astype(F32)
        out_ref[at[c]] = (scaled * gain).astype(BF16)
        gain_part = gain_part + jnp.sum((upstream * scaled).reshape(C // 8, 8, D), axis=0)
        grad = gain * upstream * inverse - mixed * factor
        grads.append(grad)
        grad_mixed_ref[at[c]] = grad
        k = k_ref[at[c]]
        high, low = split2(assoc_ref[c])
        top = lanes(v_ref[at[c]].T, high)
        rhs.append(masked_apply(grad, rows(top, top), rows(k, k, low), keep))
    turned = []
    for c in each:
        high, low = split2(solved_ref[at[c]].T)
        turned.append(lanes(high, low, high))
    part_ref[D + 72 : D + 80] = gain_part
    part_ref[D + 80 :] = jnp.zeros((D - 80, D), F32)
    adjoint = conjugate(rhs, lambda c, p: masked_apply(p, wide_ref[c], tall_ref[c], keep))
    total = None
    for c in each:
        adjoint_ref[at[c]] = adjoint[c]
        high, low = split2(lanes(grads[c], adjoint[c]))
        term = mm(turned[c], rows(high, high, low))
        total = term if total is None else total + term
    part_ref[:D] = total[:, :D].T
    pairs = total[:, D:] + total[:, D:].T
    part_ref[D : D + 64] = pack(pairs)
    diagonal = jnp.sum(jnp.where(iota2(0) == iota2(1), pairs, 0.0), axis=0, keepdims=True)
    part_ref[D + 64 : D + 72] = jnp.broadcast_to(diagonal, (8, D))


def local_kernel(k_ref, v_ref, solved_ref, adjoint_ref, grad_mixed_ref, scaled_ref,
                 grad_k_ref, grad_v_ref, out_ref, grad_q_ref):
    out_ref[...] = scaled_ref[...]
    grad_q_ref[...] = adjoint_ref[...].astype(BF16)
    chunks = k_ref.shape[0] // C
    keep = iota2(0) <= iota2(1)
    suffix = pairs = None
    for c in reversed(range(chunks)):
        at = slice(C * c, C * c + C)
        k = k_ref[at]
        v = v_ref[at]
        solved, adjoint, grad = solved_ref[at], adjoint_ref[at], grad_mixed_ref[at]
        s_high, s_low = split2(solved)
        a_high, a_low = split2(adjoint)
        g_high, g_low = split2(grad)
        st_high, st_low = split2(solved.T)
        at_high, at_low = split2(adjoint.T)
        gt_high, gt_low = split2(grad.T)
        both = mm(lanes(k, k), rows(lanes(st_high, at_high), lanes(st_low, at_low)))
        value_grad = mm(lanes(v, v), rows(gt_high, gt_low))
        key_solved = jnp.where(keep, both[:, :C], 0.0)
        other = jnp.where(keep, value_grad - both[:, C:], 0.0)
        ks_high, ks_low = split2(key_solved)
        o_high, o_low = split2(other)
        grad_v = mm(lanes(ks_high, ks_low, ks_high), rows(g_high, g_high, g_low))
        grad_k = mm(lanes(o_high, o_low, o_high), rows(s_high, s_high, s_low)) - mm(
            lanes(ks_high, ks_low, ks_high), rows(a_high, a_high, a_low)
        )
        if suffix is not None:
            more_k, more_v = finish(k, v, suffix, pairs)
            grad_k = grad_k + more_k
            grad_v = grad_v + more_v
        grad_k_ref[at] = grad_k
        grad_v_ref[at] = grad_v
        if c > 0:
            left_high, left_low = rows(gt_high, at_high), rows(gt_low, at_low)
            term = mm(lanes(left_high, left_low, left_high), rows(s_high, s_high, s_low))
            pair = term[D:] + term[D:].T
            suffix = term[:D] if suffix is None else suffix + term[:D]
            pairs = pair if pairs is None else pairs + pair


def key_weights(suffix, pairs):
    return rows(*split2(suffix), *split2(-pairs))


def finish(k, v, suffix, pairs):
    t_high, t_low = split2(suffix.T)
    return mm(lanes(v, v, k, k), key_weights(suffix, pairs)), mm(lanes(k, k), rows(t_high, t_low))


def last_kernel(k_ref, v_ref, state_ref, local_k_ref, local_v_ref, grad_k_hbm, grad_v_hbm, gain_ref,
                grad_k_ref, grad_v_ref, sem):
    suffix = state_ref[:D]
    pairs = unpack(state_ref[D : D + 64], state_ref[D + 64 : D + 65])
    half = k_ref.shape[0] // 2
    copies = []
    t_high, t_low = split2(suffix.T)
    turned = rows(t_high, t_low)
    direct = key_weights(suffix, pairs)
    for n in range(2):
        at = pl.ds(half * n, half)
        k = k_ref[at]
        grad_v_ref[at] = (local_v_ref[at] + mm(lanes(k, k), turned)).astype(BF16)
        copies.append(pltpu.make_async_copy(grad_v_ref.at[at], grad_v_hbm.at[at], sem.at[n, 0]))
        copies[-1].start()
    for n in range(2):
        at = pl.ds(half * n, half)
        k, v = k_ref[at], v_ref[at]
        grad_k_ref[at] = (local_k_ref[at] + mm(lanes(v, v, k, k), direct)).astype(BF16)
        copies.append(pltpu.make_async_copy(grad_k_ref.at[at], grad_k_hbm.at[at], sem.at[n, 1]))
        copies[-1].start()
    gain_ref[...] = jnp.sum(state_ref[D + 72 : D + 80], axis=0, keepdims=True)
    for copy in copies:
        copy.wait()


def exchange(array, axis):
    return lax.all_to_all(array, axis, split_axis=0, concat_axis=0, tiled=True)


def scan_over_seq(kernel, parts):
    slices = (SLICES, 8, D)
    held = exchange(parts.reshape(slices), SEQ)
    (held,) = call(kernel, [(slices, F32)], [VMEM], (held,), 10**5)
    return exchange(held, SEQ).reshape(2 * D, D)


def per_device(queries, keys, values, ridge, gain, grad_out):
    tok = queries.shape[0]
    chunks = tok // C
    token = (tok, D)
    state_shape = ((2 * D, D), F32)

    gain_row = gain.reshape(1, D)
    (parts,) = call(
        gram_kernel, [state_shape], [HBM] * 2, (keys, values), 4 * tok * D * D, grant=55000,
        scratch=[pltpu.VMEM(token, BF16), pltpu.VMEM(token, BF16), pltpu.SemaphoreType.DMA((2, 2))],
    )
    ridge_row = jnp.broadcast_to(ridge.reshape(1, 1), (1, D))
    parts, ridge_row = lax.optimization_barrier((parts, ridge_row))
    state = scan_over_seq(before_kernel, parts)
    solved, mixed, sums, wide, tall, assoc = call(
        forward_kernel,
        [(token, F32), (token, F32), ((HEADS, 8, D), F32),
         ((chunks, 2 * C, 2 * D), BF16), ((chunks, 3 * C, D), BF16), ((chunks, D, D), F32)],
        [VMEM] * 7,
        (ridge_row, gain_row, queries, keys, values, grad_out, state),
        10**9,
    )
    sums = exchange(sums, "head")
    scaled, adjoint, grad_mixed, parts = call(
        adjoint_kernel,
        [(token, BF16), (token, F32), (token, F32), state_shape],
        [VMEM] * 10,
        (gain_row, keys, values, grad_out, sums, solved, mixed, wide, tall, assoc),
        10**9,
    )
    local_k, local_v, output, grad_q = call(
        local_kernel,
        [(token, F32), (token, F32), (token, BF16), (token, BF16)],
        [VMEM] * 6,
        (keys, values, solved, adjoint, grad_mixed, scaled),
        5 * 10**8,
    )
    state = scan_over_seq(after_kernel, parts)
    grad_k, grad_v, grad_gain = call(
        last_kernel, [(token, BF16), (token, BF16), ((1, D), F32)], [VMEM] * 5,
        (keys, values, state, local_k, local_v), 10**8,
        scratch=[pltpu.VMEM(token, BF16), pltpu.VMEM(token, BF16), pltpu.SemaphoreType.DMA((2, 2))],
        places=[HBM, HBM, VMEM],
    )
    return output, grad_q, grad_k, grad_v, grad_gain.reshape(D)


def solution(mesh):
    split = Mesh(mesh.devices.reshape(ZN, XN, mesh.shape["head"]), ("z", "x", "head"))
    tokens = P(SEQ, "head")
    return jax.shard_map(
        per_device,
        mesh=split,
        in_specs=(tokens, tokens, tokens, P("head"), P("head"), tokens),
        out_specs=(tokens, tokens, tokens, tokens, P("head")),
        check_vma=False,
    )
```

```python
import jax
import jax.numpy as jnp
from jax import lax
from jax.experimental import pallas as pl
from jax.experimental.pallas import tpu as pltpu
from jax.sharding import Mesh
from jax.sharding import PartitionSpec as P

HEADS = 8
D = 128
CG_STEPS = 6
EPS = 1e-06
ZN = 8
XN = 4
SLICES = ZN * XN
GAIN_SLICE = 25
SEQ = ("z", "x")
C = 128
F32 = jnp.float32
BF16 = jnp.bfloat16
VMEM = pl.BlockSpec(memory_space=pltpu.VMEM)
HBM = pl.BlockSpec(memory_space=pltpu.HBM)


def split2(x):
    high = x.astype(BF16)
    return high, (x - high.astype(F32)).astype(BF16)


def mm(left, right):
    return jnp.dot(left, right, preferred_element_type=F32)


def mm_t(left, right):
    return lax.dot_general(left, right, (((0,), (0,)), ((), ())), preferred_element_type=F32)


def lanes(*parts):
    return jnp.concatenate(parts, axis=1)


def rows(*parts):
    return jnp.concatenate(parts, axis=0)


def iota2(axis):
    return lax.broadcasted_iota(jnp.int32, (C, C), axis)


def row_sum(x):
    return jnp.sum(x, axis=-1, keepdims=True)


def call(kernel, outs, ins, args, flops, grant=8192, scratch=()):
    size = sum(a.size * a.dtype.itemsize for a in args)
    return pl.pallas_call(
        kernel,
        out_shape=[jax.ShapeDtypeStruct(s, t) for s, t in outs],
        in_specs=ins,
        out_specs=[VMEM] * len(outs),
        scratch_shapes=list(scratch),
        compiler_params=pltpu.CompilerParams(vmem_limit_bytes=grant * 2**10),
        cost_estimate=pl.CostEstimate(flops=flops, bytes_accessed=size, transcendentals=0),
    )(*args)


def masked_apply(left, wide, tall, keep):
    high, low = split2(left)
    both = mm(lanes(high, low), wide)
    inner = jnp.where(keep, both[:, :C], 0.0)
    s_high, s_low = split2(inner)
    return both[:, C:] + mm(lanes(s_high, s_low, high), tall)


def conjugate(rhs, wide_ref, tall_ref, keep):
    each = range(len(rhs))
    sol = [None] * len(rhs)
    res = list(rhs)
    sea = list(rhs)
    now = [row_sum(r * r) for r in res]
    res_wide = [mm(lanes(*split2(r)), wide_ref[c]) for c, r in enumerate(res)]
    sea_wide = list(res_wide)
    for step in range(CG_STEPS):
        last = step == CG_STEPS - 1
        image = []
        for c in each:
            inner = jnp.where(keep, sea_wide[c][:, :C], 0.0)
            s_high, s_low = split2(inner)
            image.append(sea_wide[c][:, C:] + mm(lanes(s_high, s_low, sea[c].astype(BF16)), tall_ref[c]))
        if not last:
            image_wide = [mm(lanes(*split2(image[c])), wide_ref[c]) for c in each]
        alpha = [now[c] / (row_sum(sea[c] * image[c]) + EPS) for c in each]
        sol = [alpha[c] * sea[c] if step == 0 else sol[c] + alpha[c] * sea[c] for c in each]
        if last:
            break
        res = [res[c] - alpha[c] * image[c] for c in each]
        new = [row_sum(res[c] * res[c]) for c in each]
        beta = [new[c] / (now[c] + EPS) for c in each]
        sea = [res[c] + beta[c] * sea[c] for c in each]
        res_wide = [res_wide[c] - alpha[c] * image_wide[c] for c in each]
        sea_wide = [res_wide[c] + beta[c] * sea_wide[c] for c in each]
        now = new
    return sol


def gram_kernel(k_hbm, v_hbm, out_ref, k_ref, v_ref, sem):
    half = k_hbm.shape[0] // 2
    at = [pl.ds(half * n, half) for n in range(2)]
    copies = [
        pltpu.make_async_copy(source.at[at[n]], target.at[at[n]], sem.at[n, m])
        for n in range(2)
        for m, (source, target) in enumerate(((k_hbm, k_ref), (v_hbm, v_ref)))
    ]
    for copy in copies:
        copy.start()
    total = None
    for n in range(2):
        copies[2 * n].wait()
        copies[2 * n + 1].wait()
        k = k_ref[at[n]]
        term = mm_t(lanes(k, v_ref[at[n]]), k)
        total = term if total is None else total + term
    out_ref[...] = total


def before_kernel(a_ref, out_ref):
    run = jnp.zeros((8, D), F32)
    for k in range(SLICES):
        out_ref[k] = run
        run = run + a_ref[k]


def after_kernel(a_ref, out_ref):
    total = a_ref[0]
    for k in range(1, SLICES):
        total = total + a_ref[k]
    whole = lax.axis_index("z") * XN + lax.axis_index("x") == GAIN_SLICE
    run = jnp.zeros((8, D), F32)
    for k in reversed(range(SLICES)):
        out_ref[k] = jnp.where(whole, total, run)
        run = run + a_ref[k]


def pack(pairs):
    row = lax.broadcasted_iota(jnp.int32, (C // 2, C), 0)
    col = lax.broadcasted_iota(jnp.int32, (C // 2, C), 1)
    turned = pltpu.roll(pairs[C // 2 :], C // 2, 1)
    return jnp.where((col < C // 2) & (col > row), turned, pairs[: C // 2])


def unpack(packed, diagonal):
    row, col = iota2(0), iota2(1)
    half = C // 2
    both = rows(packed, pltpu.roll(packed, half, 1))
    direct = ((row < half) & ((col >= half) | (row >= col))) | ((row >= half) & (col >= half) & (row < col))
    return jnp.where(row == col, diagonal, jnp.where(direct, both, both.T))


def forward_kernel(ridge_ref, gain_ref, q_ref, k_ref, v_ref, g_ref, state_ref,
                   solved_ref, mixed_ref, sums_ref, wide_ref, tall_ref, assoc_ref):
    chunks = q_ref.shape[0] // C
    each = range(chunks)
    at = [slice(C * c, C * c + C) for c in each]
    keep = iota2(0) >= iota2(1)
    eye = iota2(0) == iota2(1)
    gram = state_ref[:D] + jnp.where(eye, ridge_ref[...], 0.0)
    assoc = state_ref[D:]
    turned = []
    for c in each:
        k = k_ref[at[c]]
        v = v_ref[at[c]]
        k_t = k.T
        turned.append(k_t)
        high, low = split2(gram)
        top = lanes(k_t, high)
        wide_ref[c, :C] = top
        wide_ref[c, C:] = top
        tall_ref[c] = rows(k, k, low)
        assoc_ref[c] = assoc
        if c < chunks - 1:
            more = mm(rows(k_t, v.T), k)
            gram = gram + more[:C]
            assoc = assoc + more[C:]
    solved = conjugate(
        [q_ref[at[c]].astype(F32) for c in each], wide_ref, tall_ref, keep
    )
    gain = gain_ref[...]
    ones = jnp.ones((8, 2 * D), BF16)
    for c in each:
        high, low = split2(assoc_ref[c].T)
        top = lanes(turned[c], high)
        v = v_ref[at[c]]
        mixed = masked_apply(solved[c], rows(top, top), rows(v, v, low), keep)
        solved_ref[at[c]] = solved[c]
        mixed_ref[at[c]] = mixed
        square = mixed * mixed
        cross = gain * g_ref[at[c]].astype(F32) * mixed
        for n, x in enumerate((square, cross)):
            total = lax.dot_general(
                ones, lanes(*split2(x)), (((1,), (1,)), ((), ())), preferred_element_type=F32
            )
            row = 4 * n + c
            for h in range(HEADS):
                sums_ref[h, row : row + 1] = total[:1]


def adjoint_kernel(gain_ref, k_ref, v_ref, g_ref, sums_ref, solved_ref, mixed_ref, wide_ref, tall_ref, assoc_ref,
                   out_ref, adjoint_ref, grad_mixed_ref, part_ref):
    chunks = k_ref.shape[0] // C
    each = range(chunks)
    at = [slice(C * c, C * c + C) for c in each]
    keep = iota2(0) >= iota2(1)
    gain = gain_ref[...]
    sums = sums_ref[0]
    for h in range(1, HEADS):
        sums = sums + sums_ref[h]
    columns = rows(sums, jnp.zeros((C - 8, C), F32)).T
    rhs = []
    gain_part = jnp.zeros((8, D), F32)
    grads = []
    for c in each:
        denom = jnp.sqrt(columns[:, c : c + 1] / (HEADS * D) + EPS)
        inverse = 1.0 / denom
        factor = columns[:, 4 + c : 5 + c] / (denom * denom * denom * (HEADS * D))
        mixed = mixed_ref[at[c]]
        scaled = mixed * inverse
        upstream = g_ref[at[c]].astype(F32)
        out_ref[at[c]] = (scaled * gain).astype(BF16)
        gain_part = gain_part + jnp.sum((upstream * scaled).reshape(C // 8, 8, D), axis=0)
        grad = gain * upstream * inverse - mixed * factor
        grads.append(grad)
        grad_mixed_ref[at[c]] = grad
        k = k_ref[at[c]]
        high, low = split2(assoc_ref[c])
        top = lanes(v_ref[at[c]].T, high)
        rhs.append(masked_apply(grad, rows(top, top), rows(k, k, low), keep))
    turned = []
    for c in each:
        high, low = split2(solved_ref[at[c]].T)
        turned.append(lanes(high, low, high))
    part_ref[D + 72 : D + 80] = gain_part
    part_ref[D + 80 :] = jnp.zeros((D - 80, D), F32)
    adjoint = conjugate(rhs, wide_ref, tall_ref, keep)
    total = None
    for c in each:
        adjoint_ref[at[c]] = adjoint[c]
        high, low = split2(lanes(grads[c], adjoint[c]))
        term = mm(turned[c], rows(high, high, low))
        total = term if total is None else total + term
    part_ref[:D] = total[:, :D].T
    pairs = total[:, D:] + total[:, D:].T
    part_ref[D : D + 64] = pack(pairs)
    diagonal = jnp.sum(jnp.where(iota2(0) == iota2(1), pairs, 0.0), axis=0, keepdims=True)
    part_ref[D + 64 : D + 72] = jnp.broadcast_to(diagonal, (8, D))


def local_kernel(k_ref, v_ref, solved_ref, adjoint_ref, grad_mixed_ref, scaled_ref,
                 grad_k_ref, grad_v_ref, out_ref, grad_q_ref):
    out_ref[...] = scaled_ref[...]
    grad_q_ref[...] = adjoint_ref[...].astype(BF16)
    chunks = k_ref.shape[0] // C
    keep = iota2(0) <= iota2(1)
    suffix = pairs = None
    for c in reversed(range(chunks)):
        at = slice(C * c, C * c + C)
        k = k_ref[at]
        v = v_ref[at]
        solved, adjoint, grad = solved_ref[at], adjoint_ref[at], grad_mixed_ref[at]
        s_high, s_low = split2(solved)
        a_high, a_low = split2(adjoint)
        g_high, g_low = split2(grad)
        st_high, st_low = split2(solved.T)
        at_high, at_low = split2(adjoint.T)
        gt_high, gt_low = split2(grad.T)
        both = mm(lanes(k, k), rows(lanes(st_high, at_high), lanes(st_low, at_low)))
        value_grad = mm(lanes(v, v), rows(gt_high, gt_low))
        key_solved = jnp.where(keep, both[:, :C], 0.0)
        other = jnp.where(keep, value_grad - both[:, C:], 0.0)
        ks_high, ks_low = split2(key_solved)
        o_high, o_low = split2(other)
        grad_v = mm(lanes(ks_high, ks_low, ks_high), rows(g_high, g_high, g_low))
        grad_k = mm(lanes(o_high, o_low, o_high), rows(s_high, s_high, s_low)) - mm(
            lanes(ks_high, ks_low, ks_high), rows(a_high, a_high, a_low)
        )
        if suffix is not None:
            more_k, more_v = finish(k, v, suffix, pairs)
            grad_k = grad_k + more_k
            grad_v = grad_v + more_v
        grad_k_ref[at] = grad_k
        grad_v_ref[at] = grad_v
        if c > 0:
            left_high, left_low = rows(gt_high, at_high), rows(gt_low, at_low)
            term = mm(lanes(left_high, left_low, left_high), rows(s_high, s_high, s_low))
            pair = term[D:] + term[D:].T
            suffix = term[:D] if suffix is None else suffix + term[:D]
            pairs = pair if pairs is None else pairs + pair


def finish(k, v, suffix, pairs):
    t_high, t_low = split2(suffix.T)
    weights = rows(*split2(suffix), *split2(-pairs))
    return mm(lanes(v, v, k, k), weights), mm(lanes(k, k), rows(t_high, t_low))


def last_kernel(k_ref, v_ref, state_ref, local_k_ref, local_v_ref, grad_k_ref, grad_v_ref, gain_ref):
    pairs = unpack(state_ref[D : D + 64], state_ref[D + 64 : D + 65])
    grad_k, grad_v = finish(k_ref[...], v_ref[...], state_ref[:D], pairs)
    grad_v_ref[...] = (local_v_ref[...] + grad_v).astype(BF16)
    grad_k_ref[...] = (local_k_ref[...] + grad_k).astype(BF16)
    gain_ref[...] = jnp.sum(state_ref[D + 72 : D + 80], axis=0, keepdims=True)


def exchange(array, axis):
    return lax.all_to_all(array, axis, split_axis=0, concat_axis=0, tiled=True)


def scan_over_seq(kernel, parts):
    slices = (SLICES, 8, D)
    held = exchange(parts.reshape(slices), SEQ)
    (held,) = call(kernel, [(slices, F32)], [VMEM], (held,), 10**5)
    return exchange(held, SEQ).reshape(2 * D, D)


def per_device(queries, keys, values, ridge, gain, grad_out):
    tok = queries.shape[0]
    chunks = tok // C
    token = (tok, D)
    state_shape = ((2 * D, D), F32)

    gain_row = gain.reshape(1, D)
    (parts,) = call(
        gram_kernel, [state_shape], [HBM] * 2, (keys, values), 4 * tok * D * D, grant=55000,
        scratch=[pltpu.VMEM(token, BF16), pltpu.VMEM(token, BF16), pltpu.SemaphoreType.DMA((2, 2))],
    )
    ridge_row = jnp.broadcast_to(ridge.reshape(1, 1), (1, D))
    parts, ridge_row = lax.optimization_barrier((parts, ridge_row))
    state = scan_over_seq(before_kernel, parts)
    solved, mixed, sums, wide, tall, assoc = call(
        forward_kernel,
        [(token, F32), (token, F32), ((HEADS, 8, D), F32),
         ((chunks, 2 * C, 2 * D), BF16), ((chunks, 3 * C, D), BF16), ((chunks, D, D), F32)],
        [VMEM] * 7,
        (ridge_row, gain_row, queries, keys, values, grad_out, state),
        10**9,
    )
    sums = exchange(sums, ("core", "y"))
    scaled, adjoint, grad_mixed, parts = call(
        adjoint_kernel,
        [(token, BF16), (token, F32), (token, F32), state_shape],
        [VMEM] * 10,
        (gain_row, keys, values, grad_out, sums, solved, mixed, wide, tall, assoc),
        10**9,
    )
    local_k, local_v, output, grad_q = call(
        local_kernel,
        [(token, F32), (token, F32), (token, BF16), (token, BF16)],
        [VMEM] * 6,
        (keys, values, solved, adjoint, grad_mixed, scaled),
        5 * 10**8,
    )
    state = scan_over_seq(after_kernel, parts)
    grad_k, grad_v, grad_gain = call(
        last_kernel, [(token, BF16), (token, BF16), ((1, D), F32)], [VMEM] * 5,
        (keys, values, state, local_k, local_v), 10**8,
    )
    return output, grad_q, grad_k, grad_v, grad_gain.reshape(D)


def solution(mesh):
    split = Mesh(mesh.devices.reshape(ZN, XN, mesh.shape["head"] // 2, 2), ("z", "x", "y", "core"))
    head = ("y", "core")
    tokens = P(SEQ, head)
    return jax.shard_map(
        per_device,
        mesh=split,
        in_specs=(tokens, tokens, tokens, P(head), P(head), tokens),
        out_specs=(tokens, tokens, tokens, tokens, P(head)),
        check_vma=False,
    )
```

```python
import jax
import jax.numpy as jnp
from jax import lax
from jax.experimental import pallas as pl
from jax.experimental.pallas import tpu as pltpu
from jax.sharding import Mesh
from jax.sharding import PartitionSpec as P

HEADS = 8
D = 128
CG_STEPS = 6
EPS = 1e-06
ZN = 8
XN = 4
SLICES = ZN * XN
GAIN_SLICE = 25
SEQ = ("z", "x")
C = 128
F32 = jnp.float32
BF16 = jnp.bfloat16
VMEM = pl.BlockSpec(memory_space=pltpu.VMEM)
HBM = pl.BlockSpec(memory_space=pltpu.HBM)


def split2(x):
    high = x.astype(BF16)
    return high, (x - high.astype(F32)).astype(BF16)


def mm(left, right):
    return jnp.dot(left, right, preferred_element_type=F32)


def mm_t(left, right):
    return lax.dot_general(left, right, (((0,), (0,)), ((), ())), preferred_element_type=F32)


def lanes(*parts):
    return jnp.concatenate(parts, axis=1)


def rows(*parts):
    return jnp.concatenate(parts, axis=0)


def iota2(axis):
    return lax.broadcasted_iota(jnp.int32, (C, C), axis)


def row_sum(x):
    return jnp.sum(x, axis=-1, keepdims=True)


def call(kernel, outs, ins, args, flops, grant=8192, scratch=()):
    size = sum(a.size * a.dtype.itemsize for a in args)
    return pl.pallas_call(
        kernel,
        out_shape=[jax.ShapeDtypeStruct(s, t) for s, t in outs],
        in_specs=ins,
        out_specs=[VMEM] * len(outs),
        scratch_shapes=list(scratch),
        compiler_params=pltpu.CompilerParams(vmem_limit_bytes=grant * 2**10),
        cost_estimate=pl.CostEstimate(flops=flops, bytes_accessed=size, transcendentals=0),
    )(*args)


def masked_apply(left, wide, tall, keep):
    high, low = split2(left)
    both = mm(lanes(high, low), wide)
    inner = jnp.where(keep, both[:, :C], 0.0)
    s_high, s_low = split2(inner)
    return both[:, C:] + mm(lanes(s_high, s_low, high), tall)


def conjugate(rhs, wide_ref, tall_ref, keep, with_inner=False):
    each = range(len(rhs))
    sol = [None] * len(rhs)
    res = list(rhs)
    sea = list(rhs)
    now = [row_sum(r * r) for r in res]
    res_wide = [mm(lanes(*split2(r)), wide_ref[c]) for c, r in enumerate(res)]
    sea_wide = list(res_wide)
    sol_inner = [None] * len(rhs)
    for step in range(CG_STEPS):
        last = step == CG_STEPS - 1
        image = []
        for c in each:
            inner = jnp.where(keep, sea_wide[c][:, :C], 0.0)
            s_high, s_low = split2(inner)
            image.append(sea_wide[c][:, C:] + mm(lanes(s_high, s_low, sea[c].astype(BF16)), tall_ref[c]))
        if not last:
            image_wide = [mm(lanes(*split2(image[c])), wide_ref[c]) for c in each]
        alpha = [now[c] / (row_sum(sea[c] * image[c]) + EPS) for c in each]
        sol = [alpha[c] * sea[c] if step == 0 else sol[c] + alpha[c] * sea[c] for c in each]
        if with_inner:
            inner = [alpha[c] * sea_wide[c][:, :C] for c in each]
            sol_inner = inner if step == 0 else [sol_inner[c] + inner[c] for c in each]
        if last:
            break
        res = [res[c] - alpha[c] * image[c] for c in each]
        new = [row_sum(res[c] * res[c]) for c in each]
        beta = [new[c] / (now[c] + EPS) for c in each]
        sea = [res[c] + beta[c] * sea[c] for c in each]
        res_wide = [res_wide[c] - alpha[c] * image_wide[c] for c in each]
        sea_wide = [res_wide[c] + beta[c] * sea_wide[c] for c in each]
        now = new
    return sol, sol_inner


def gram_kernel(k_hbm, v_hbm, out_ref, k_ref, v_ref, sem):
    half = k_hbm.shape[0] // 2
    at = [pl.ds(half * n, half) for n in range(2)]
    copies = [
        pltpu.make_async_copy(source.at[at[n]], target.at[at[n]], sem.at[n, m])
        for n in range(2)
        for m, (source, target) in enumerate(((k_hbm, k_ref), (v_hbm, v_ref)))
    ]
    for copy in copies:
        copy.start()
    total = None
    for n in range(2):
        copies[2 * n].wait()
        copies[2 * n + 1].wait()
        k = k_ref[at[n]]
        term = mm_t(lanes(k, v_ref[at[n]]), k)
        total = term if total is None else total + term
    out_ref[...] = total


def before_kernel(a_ref, out_ref):
    run = jnp.zeros((8, D), F32)
    for k in range(SLICES):
        out_ref[k] = run
        run = run + a_ref[k]


def after_kernel(a_ref, out_ref):
    total = a_ref[0]
    for k in range(1, SLICES):
        total = total + a_ref[k]
    whole = lax.axis_index("z") * XN + lax.axis_index("x") == GAIN_SLICE
    run = jnp.zeros((8, D), F32)
    for k in reversed(range(SLICES)):
        out_ref[k] = jnp.where(whole, total, run)
        run = run + a_ref[k]


def pack(pairs):
    row = lax.broadcasted_iota(jnp.int32, (C // 2, C), 0)
    col = lax.broadcasted_iota(jnp.int32, (C // 2, C), 1)
    turned = pltpu.roll(pairs[C // 2 :], C // 2, 1)
    return jnp.where((col < C // 2) & (col > row), turned, pairs[: C // 2])


def unpack(packed, diagonal):
    row, col = iota2(0), iota2(1)
    half = C // 2
    both = rows(packed, pltpu.roll(packed, half, 1))
    direct = ((row < half) & ((col >= half) | (row >= col))) | ((row >= half) & (col >= half) & (row < col))
    return jnp.where(row == col, diagonal, jnp.where(direct, both, both.T))


def forward_kernel(ridge_ref, gain_ref, q_ref, k_ref, v_ref, g_ref, state_ref,
                   solved_ref, mixed_ref, sums_ref, wide_ref, tall_ref, assoc_ref):
    chunks = q_ref.shape[0] // C
    each = range(chunks)
    at = [slice(C * c, C * c + C) for c in each]
    keep = iota2(0) >= iota2(1)
    eye = iota2(0) == iota2(1)
    gram = state_ref[:D] + jnp.where(eye, ridge_ref[...], 0.0)
    assoc = state_ref[D:]
    for c in each:
        k = k_ref[at[c]]
        v = v_ref[at[c]]
        k_t = k.T
        high, low = split2(gram)
        top = lanes(k_t, high)
        wide_ref[c, :C] = top
        wide_ref[c, C:] = top
        tall_ref[c] = rows(k, k, low)
        assoc_ref[c] = assoc
        if c < chunks - 1:
            more = mm(rows(k_t, v.T), k)
            gram = gram + more[:C]
            assoc = assoc + more[C:]
    weights = []
    for c in each:
        v = v_ref[at[c]]
        high, low = split2(assoc_ref[c].T)
        weights.append(rows(v, v, high, high, low))
    solved, inner = conjugate(
        [q_ref[at[c]].astype(F32) for c in each], wide_ref, tall_ref, keep, True
    )
    gain = gain_ref[...]
    ones = jnp.ones((8, 2 * D), BF16)
    for c in each:
        x_high, x_low = split2(solved[c])
        s_high, s_low = split2(jnp.where(keep, inner[c], 0.0))
        mixed = mm(lanes(s_high, s_low, x_high, x_low, x_high), weights[c])
        solved_ref[at[c]] = solved[c]
        mixed_ref[at[c]] = mixed
        square = mixed * mixed
        cross = gain * g_ref[at[c]].astype(F32) * mixed
        for n, x in enumerate((square, cross)):
            total = lax.dot_general(
                ones, lanes(*split2(x)), (((1,), (1,)), ((), ())), preferred_element_type=F32
            )
            row = 4 * n + c
            for h in range(HEADS):
                sums_ref[h, row : row + 1] = total[:1]


def adjoint_kernel(gain_ref, k_ref, v_ref, g_ref, sums_ref, solved_ref, mixed_ref, wide_ref, tall_ref, assoc_ref,
                   out_ref, adjoint_ref, grad_mixed_ref, part_ref):
    chunks = k_ref.shape[0] // C
    each = range(chunks)
    at = [slice(C * c, C * c + C) for c in each]
    keep = iota2(0) >= iota2(1)
    gain = gain_ref[...]
    sums = sums_ref[0]
    for h in range(1, HEADS):
        sums = sums + sums_ref[h]
    columns = rows(sums, jnp.zeros((C - 8, C), F32)).T
    rhs = []
    gain_part = jnp.zeros((8, D), F32)
    grads = []
    for c in each:
        denom = jnp.sqrt(columns[:, c : c + 1] / (HEADS * D) + EPS)
        inverse = 1.0 / denom
        factor = columns[:, 4 + c : 5 + c] / (denom * denom * denom * (HEADS * D))
        mixed = mixed_ref[at[c]]
        scaled = mixed * inverse
        upstream = g_ref[at[c]].astype(F32)
        out_ref[at[c]] = (scaled * gain).astype(BF16)
        gain_part = gain_part + jnp.sum((upstream * scaled).reshape(C // 8, 8, D), axis=0)
        grad = gain * upstream * inverse - mixed * factor
        grads.append(grad)
        grad_mixed_ref[at[c]] = grad
        k = k_ref[at[c]]
        high, low = split2(assoc_ref[c])
        top = lanes(v_ref[at[c]].T, high)
        rhs.append(masked_apply(grad, rows(top, top), rows(k, k, low), keep))
    turned = []
    for c in each:
        high, low = split2(solved_ref[at[c]].T)
        turned.append(lanes(high, low, high))
    part_ref[D + 72 : D + 80] = gain_part
    part_ref[D + 80 :] = jnp.zeros((D - 80, D), F32)
    adjoint, _ = conjugate(rhs, wide_ref, tall_ref, keep)
    total = None
    for c in each:
        adjoint_ref[at[c]] = adjoint[c]
        high, low = split2(lanes(grads[c], adjoint[c]))
        term = mm(turned[c], rows(high, high, low))
        total = term if total is None else total + term
    part_ref[:D] = total[:, :D].T
    pairs = total[:, D:] + total[:, D:].T
    part_ref[D : D + 64] = pack(pairs)
    diagonal = jnp.sum(jnp.where(iota2(0) == iota2(1), pairs, 0.0), axis=0, keepdims=True)
    part_ref[D + 64 : D + 72] = jnp.broadcast_to(diagonal, (8, D))


def local_kernel(k_ref, v_ref, solved_ref, adjoint_ref, grad_mixed_ref, scaled_ref,
                 grad_k_ref, grad_v_ref, out_ref, grad_q_ref):
    out_ref[...] = scaled_ref[...]
    grad_q_ref[...] = adjoint_ref[...].astype(BF16)
    chunks = k_ref.shape[0] // C
    keep = iota2(0) <= iota2(1)
    suffix = pairs = None
    for c in reversed(range(chunks)):
        at = slice(C * c, C * c + C)
        k = k_ref[at]
        v = v_ref[at]
        solved, adjoint, grad = solved_ref[at], adjoint_ref[at], grad_mixed_ref[at]
        s_high, s_low = split2(solved)
        a_high, a_low = split2(adjoint)
        g_high, g_low = split2(grad)
        st_high, st_low = split2(solved.T)
        at_high, at_low = split2(adjoint.T)
        gt_high, gt_low = split2(grad.T)
        both = mm(lanes(k, k), rows(lanes(st_high, at_high), lanes(st_low, at_low)))
        value_grad = mm(lanes(v, v), rows(gt_high, gt_low))
        key_solved = jnp.where(keep, both[:, :C], 0.0)
        other = jnp.where(keep, value_grad - both[:, C:], 0.0)
        ks_high, ks_low = split2(key_solved)
        o_high, o_low = split2(other)
        grad_v = mm(lanes(ks_high, ks_low, ks_high), rows(g_high, g_high, g_low))
        grad_k = mm(lanes(o_high, o_low, o_high), rows(s_high, s_high, s_low)) - mm(
            lanes(ks_high, ks_low, ks_high), rows(a_high, a_high, a_low)
        )
        if suffix is not None:
            more_k, more_v = finish(k, v, suffix, pairs)
            grad_k = grad_k + more_k
            grad_v = grad_v + more_v
        grad_k_ref[at] = grad_k
        grad_v_ref[at] = grad_v
        if c > 0:
            left_high, left_low = rows(gt_high, at_high), rows(gt_low, at_low)
            term = mm(lanes(left_high, left_low, left_high), rows(s_high, s_high, s_low))
            pair = term[D:] + term[D:].T
            suffix = term[:D] if suffix is None else suffix + term[:D]
            pairs = pair if pairs is None else pairs + pair


def finish(k, v, suffix, pairs):
    t_high, t_low = split2(suffix.T)
    weights = rows(*split2(suffix), *split2(-pairs))
    return mm(lanes(v, v, k, k), weights), mm(lanes(k, k), rows(t_high, t_low))


def last_kernel(k_ref, v_ref, state_ref, local_k_ref, local_v_ref, grad_k_ref, grad_v_ref, gain_ref):
    pairs = unpack(state_ref[D : D + 64], state_ref[D + 64 : D + 65])
    grad_k, grad_v = finish(k_ref[...], v_ref[...], state_ref[:D], pairs)
    grad_v_ref[...] = (local_v_ref[...] + grad_v).astype(BF16)
    grad_k_ref[...] = (local_k_ref[...] + grad_k).astype(BF16)
    gain_ref[...] = jnp.sum(state_ref[D + 72 : D + 80], axis=0, keepdims=True)


def exchange(array, axis):
    return lax.all_to_all(array, axis, split_axis=0, concat_axis=0, tiled=True)


def scan_over_seq(kernel, parts):
    slices = (SLICES, 8, D)
    held = exchange(parts.reshape(slices), SEQ)
    (held,) = call(kernel, [(slices, F32)], [VMEM], (held,), 10**5)
    return exchange(held, SEQ).reshape(2 * D, D)


def per_device(queries, keys, values, ridge, gain, grad_out):
    tok = queries.shape[0]
    chunks = tok // C
    token = (tok, D)
    state_shape = ((2 * D, D), F32)

    gain_row = gain.reshape(1, D)
    (parts,) = call(
        gram_kernel, [state_shape], [HBM] * 2, (keys, values), 4 * tok * D * D, grant=55000,
        scratch=[pltpu.VMEM(token, BF16), pltpu.VMEM(token, BF16), pltpu.SemaphoreType.DMA((2, 2))],
    )
    ridge_row = jnp.broadcast_to(ridge.reshape(1, 1), (1, D))
    parts, ridge_row = lax.optimization_barrier((parts, ridge_row))
    state = scan_over_seq(before_kernel, parts)
    solved, mixed, sums, wide, tall, assoc = call(
        forward_kernel,
        [(token, F32), (token, F32), ((HEADS, 8, D), F32),
         ((chunks, 2 * C, 2 * D), BF16), ((chunks, 3 * C, D), BF16), ((chunks, D, D), F32)],
        [VMEM] * 7,
        (ridge_row, gain_row, queries, keys, values, grad_out, state),
        10**9,
    )
    sums = exchange(sums, ("core", "y"))
    scaled, adjoint, grad_mixed, parts = call(
        adjoint_kernel,
        [(token, BF16), (token, F32), (token, F32), state_shape],
        [VMEM] * 10,
        (gain_row, keys, values, grad_out, sums, solved, mixed, wide, tall, assoc),
        10**9,
    )
    local_k, local_v, output, grad_q = call(
        local_kernel,
        [(token, F32), (token, F32), (token, BF16), (token, BF16)],
        [VMEM] * 6,
        (keys, values, solved, adjoint, grad_mixed, scaled),
        5 * 10**8,
    )
    state = scan_over_seq(after_kernel, parts)
    grad_k, grad_v, grad_gain = call(
        last_kernel, [(token, BF16), (token, BF16), ((1, D), F32)], [VMEM] * 5,
        (keys, values, state, local_k, local_v), 10**8,
    )
    return output, grad_q, grad_k, grad_v, grad_gain.reshape(D)


def solution(mesh):
    split = Mesh(mesh.devices.reshape(ZN, XN, mesh.shape["head"] // 2, 2), ("z", "x", "y", "core"))
    head = ("y", "core")
    tokens = P(SEQ, head)
    return jax.shard_map(
        per_device,
        mesh=split,
        in_specs=(tokens, tokens, tokens, P(head), P(head), tokens),
        out_specs=(tokens, tokens, tokens, tokens, P(head)),
        check_vma=False,
    )
```

```python
import jax
import jax.numpy as jnp
from jax import lax
from jax.experimental import pallas as pl
from jax.experimental.pallas import tpu as pltpu
from jax.sharding import Mesh
from jax.sharding import PartitionSpec as P

HEADS = 8
D = 128
CG_STEPS = 6
EPS = 1e-06
ZN = 8
XN = 4
SLICES = ZN * XN
GAIN_SLICE = 25
SEQ = ("z", "x")
C = 128
F32 = jnp.float32
BF16 = jnp.bfloat16
VMEM = pl.BlockSpec(memory_space=pltpu.VMEM)
HBM = pl.BlockSpec(memory_space=pltpu.HBM)


def split2(x):
    high = x.astype(BF16)
    return high, (x - high.astype(F32)).astype(BF16)


def mm(left, right):
    return jnp.dot(left, right, preferred_element_type=F32)


def mm_t(left, right):
    return lax.dot_general(left, right, (((0,), (0,)), ((), ())), preferred_element_type=F32)


def lanes(*parts):
    return jnp.concatenate(parts, axis=1)


def rows(*parts):
    return jnp.concatenate(parts, axis=0)


def iota2(axis):
    return lax.broadcasted_iota(jnp.int32, (C, C), axis)


def row_sum(x):
    return jnp.sum(x, axis=-1, keepdims=True)


def call(kernel, outs, ins, args, flops, grant=8192, scratch=()):
    size = sum(a.size * a.dtype.itemsize for a in args)
    return pl.pallas_call(
        kernel,
        out_shape=[jax.ShapeDtypeStruct(s, t) for s, t in outs],
        in_specs=ins,
        out_specs=[VMEM] * len(outs),
        scratch_shapes=list(scratch),
        compiler_params=pltpu.CompilerParams(vmem_limit_bytes=grant * 2**10),
        cost_estimate=pl.CostEstimate(flops=flops, bytes_accessed=size, transcendentals=0),
    )(*args)


def masked_apply(left, wide, tall, keep):
    high, low = split2(left)
    both = mm(lanes(high, low), wide)
    inner = jnp.where(keep, both[:, :C], 0.0)
    s_high, s_low = split2(inner)
    return both[:, C:] + mm(lanes(s_high, s_low, high), tall)


def conjugate(rhs, wide_ref, tall_ref, keep, exact=None, with_inner=False):
    each = range(len(rhs))
    sol = [None] * len(rhs)
    res = list(rhs)
    sea = list(rhs)
    now = [row_sum(r * r) for r in res]
    if exact is None:
        res_wide = [mm(lanes(*split2(r)), wide_ref[c]) for c, r in enumerate(res)]
    else:
        res_wide = [mm(r, wide_ref[c, :C]) for c, r in enumerate(exact)]
    sea_wide = list(res_wide)
    sol_inner = [None] * len(rhs)
    for step in range(CG_STEPS):
        last = step == CG_STEPS - 1
        image = []
        for c in each:
            inner = jnp.where(keep, sea_wide[c][:, :C], 0.0)
            s_high, s_low = split2(inner)
            image.append(sea_wide[c][:, C:] + mm(lanes(s_high, s_low, sea[c].astype(BF16)), tall_ref[c]))
        if not last:
            image_wide = [mm(lanes(*split2(image[c])), wide_ref[c]) for c in each]
        alpha = [now[c] / (row_sum(sea[c] * image[c]) + EPS) for c in each]
        sol = [alpha[c] * sea[c] if step == 0 else sol[c] + alpha[c] * sea[c] for c in each]
        if with_inner:
            inner = [alpha[c] * sea_wide[c][:, :C] for c in each]
            sol_inner = inner if step == 0 else [sol_inner[c] + inner[c] for c in each]
        if last:
            break
        res = [res[c] - alpha[c] * image[c] for c in each]
        new = [row_sum(res[c] * res[c]) for c in each]
        beta = [new[c] / (now[c] + EPS) for c in each]
        sea = [res[c] + beta[c] * sea[c] for c in each]
        res_wide = [res_wide[c] - alpha[c] * image_wide[c] for c in each]
        sea_wide = [res_wide[c] + beta[c] * sea_wide[c] for c in each]
        now = new
    return sol, sol_inner


def gram_kernel(k_hbm, v_hbm, out_ref, k_ref, v_ref, sem):
    half = k_hbm.shape[0] // 2
    at = [pl.ds(half * n, half) for n in range(2)]
    copies = [
        pltpu.make_async_copy(source.at[at[n]], target.at[at[n]], sem.at[n, m])
        for n in range(2)
        for m, (source, target) in enumerate(((k_hbm, k_ref), (v_hbm, v_ref)))
    ]
    for copy in copies:
        copy.start()
    total = None
    for n in range(2):
        copies[2 * n].wait()
        copies[2 * n + 1].wait()
        k = k_ref[at[n]]
        term = mm_t(lanes(k, v_ref[at[n]]), k)
        total = term if total is None else total + term
    out_ref[...] = total


def before_kernel(a_ref, out_ref):
    run = jnp.zeros((8, D), F32)
    for k in range(SLICES):
        out_ref[k] = run
        run = run + a_ref[k]


def after_kernel(a_ref, out_ref):
    total = a_ref[0]
    for k in range(1, SLICES):
        total = total + a_ref[k]
    whole = lax.axis_index("z") * XN + lax.axis_index("x") == GAIN_SLICE
    run = jnp.zeros((8, D), F32)
    for k in reversed(range(SLICES)):
        out_ref[k] = jnp.where(whole, total, run)
        run = run + a_ref[k]


def pack(pairs):
    row = lax.broadcasted_iota(jnp.int32, (C // 2, C), 0)
    col = lax.broadcasted_iota(jnp.int32, (C // 2, C), 1)
    turned = pltpu.roll(pairs[C // 2 :], C // 2, 1)
    return jnp.where((col < C // 2) & (col > row), turned, pairs[: C // 2])


def unpack(packed, diagonal):
    row, col = iota2(0), iota2(1)
    half = C // 2
    both = rows(packed, pltpu.roll(packed, half, 1))
    direct = ((row < half) & ((col >= half) | (row >= col))) | ((row >= half) & (col >= half) & (row < col))
    return jnp.where(row == col, diagonal, jnp.where(direct, both, both.T))


def forward_kernel(ridge_ref, gain_ref, q_ref, k_ref, v_ref, g_ref, state_ref,
                   solved_ref, mixed_ref, sums_ref, wide_ref, tall_ref, assoc_ref):
    chunks = q_ref.shape[0] // C
    each = range(chunks)
    at = [slice(C * c, C * c + C) for c in each]
    keep = iota2(0) >= iota2(1)
    eye = iota2(0) == iota2(1)
    gram = state_ref[:D] + jnp.where(eye, ridge_ref[...], 0.0)
    assoc = state_ref[D:]
    for c in each:
        k = k_ref[at[c]]
        v = v_ref[at[c]]
        k_t = k.T
        high, low = split2(gram)
        top = lanes(k_t, high)
        wide_ref[c, :C] = top
        wide_ref[c, C:] = top
        tall_ref[c] = rows(k, k, low)
        assoc_ref[c] = assoc
        if c < chunks - 1:
            more = mm(rows(k_t, v.T), k)
            gram = gram + more[:C]
            assoc = assoc + more[C:]
    weights = []
    for c in each:
        v = v_ref[at[c]]
        high, low = split2(assoc_ref[c].T)
        weights.append(rows(v, v, high, high, low))
    solved, inner = conjugate(
        [q_ref[at[c]].astype(F32) for c in each], wide_ref, tall_ref, keep, [q_ref[at[c]] for c in each], True
    )
    gain = gain_ref[...]
    ones = jnp.ones((8, 2 * D), BF16)
    for c in each:
        x_high, x_low = split2(solved[c])
        s_high, s_low = split2(jnp.where(keep, inner[c], 0.0))
        mixed = mm(lanes(s_high, s_low, x_high, x_low, x_high), weights[c])
        solved_ref[at[c]] = solved[c]
        mixed_ref[at[c]] = mixed
        square = mixed * mixed
        cross = gain * g_ref[at[c]].astype(F32) * mixed
        for n, x in enumerate((square, cross)):
            total = lax.dot_general(
                ones, lanes(*split2(x)), (((1,), (1,)), ((), ())), preferred_element_type=F32
            )
            row = 4 * n + c
            for h in range(HEADS):
                sums_ref[h, row : row + 1] = total[:1]


def adjoint_kernel(gain_ref, k_ref, v_ref, g_ref, sums_ref, solved_ref, mixed_ref, wide_ref, tall_ref, assoc_ref,
                   out_ref, adjoint_ref, grad_mixed_ref, part_ref):
    chunks = k_ref.shape[0] // C
    each = range(chunks)
    at = [slice(C * c, C * c + C) for c in each]
    keep = iota2(0) >= iota2(1)
    gain = gain_ref[...]
    sums = sums_ref[0]
    for h in range(1, HEADS):
        sums = sums + sums_ref[h]
    columns = rows(sums, jnp.zeros((C - 8, C), F32)).T
    rhs = []
    gain_part = jnp.zeros((8, D), F32)
    grads = []
    for c in each:
        denom = jnp.sqrt(columns[:, c : c + 1] / (HEADS * D) + EPS)
        inverse = 1.0 / denom
        factor = columns[:, 4 + c : 5 + c] / (denom * denom * denom * (HEADS * D))
        mixed = mixed_ref[at[c]]
        scaled = mixed * inverse
        upstream = g_ref[at[c]].astype(F32)
        out_ref[at[c]] = (scaled * gain).astype(BF16)
        gain_part = gain_part + jnp.sum((upstream * scaled).reshape(C // 8, 8, D), axis=0)
        grad = gain * upstream * inverse - mixed * factor
        grads.append(grad)
        grad_mixed_ref[at[c]] = grad
        k = k_ref[at[c]]
        high, low = split2(assoc_ref[c])
        top = lanes(v_ref[at[c]].T, high)
        rhs.append(masked_apply(grad, rows(top, top), rows(k, k, low), keep))
    turned = []
    for c in each:
        high, low = split2(solved_ref[at[c]].T)
        turned.append(lanes(high, low, high))
    part_ref[D + 72 : D + 80] = gain_part
    part_ref[D + 80 :] = jnp.zeros((D - 80, D), F32)
    adjoint, _ = conjugate(rhs, wide_ref, tall_ref, keep)
    total = None
    for c in each:
        adjoint_ref[at[c]] = adjoint[c]
        high, low = split2(lanes(grads[c], adjoint[c]))
        term = mm(turned[c], rows(high, high, low))
        total = term if total is None else total + term
    part_ref[:D] = total[:, :D].T
    pairs = total[:, D:] + total[:, D:].T
    part_ref[D : D + 64] = pack(pairs)
    diagonal = jnp.sum(jnp.where(iota2(0) == iota2(1), pairs, 0.0), axis=0, keepdims=True)
    part_ref[D + 64 : D + 72] = jnp.broadcast_to(diagonal, (8, D))


def local_kernel(k_ref, v_ref, solved_ref, adjoint_ref, grad_mixed_ref, scaled_ref,
                 grad_k_ref, grad_v_ref, out_ref, grad_q_ref):
    out_ref[...] = scaled_ref[...]
    grad_q_ref[...] = adjoint_ref[...].astype(BF16)
    chunks = k_ref.shape[0] // C
    keep = iota2(0) <= iota2(1)
    suffix = pairs = None
    for c in reversed(range(chunks)):
        at = slice(C * c, C * c + C)
        k = k_ref[at]
        v = v_ref[at]
        solved, adjoint, grad = solved_ref[at], adjoint_ref[at], grad_mixed_ref[at]
        s_high, s_low = split2(solved)
        a_high, a_low = split2(adjoint)
        g_high, g_low = split2(grad)
        st_high, st_low = split2(solved.T)
        at_high, at_low = split2(adjoint.T)
        gt_high, gt_low = split2(grad.T)
        both = mm(lanes(k, k), rows(lanes(st_high, at_high), lanes(st_low, at_low)))
        value_grad = mm(lanes(v, v), rows(gt_high, gt_low))
        key_solved = jnp.where(keep, both[:, :C], 0.0)
        other = jnp.where(keep, value_grad - both[:, C:], 0.0)
        ks_high, ks_low = split2(key_solved)
        o_high, o_low = split2(other)
        grad_v = mm(lanes(ks_high, ks_low, ks_high), rows(g_high, g_high, g_low))
        grad_k = mm(lanes(o_high, o_low, o_high), rows(s_high, s_high, s_low)) - mm(
            lanes(ks_high, ks_low, ks_high), rows(a_high, a_high, a_low)
        )
        if suffix is not None:
            more_k, more_v = finish(k, v, suffix, pairs)
            grad_k = grad_k + more_k
            grad_v = grad_v + more_v
        grad_k_ref[at] = grad_k
        grad_v_ref[at] = grad_v
        if c > 0:
            left_high, left_low = rows(gt_high, at_high), rows(gt_low, at_low)
            term = mm(lanes(left_high, left_low, left_high), rows(s_high, s_high, s_low))
            pair = term[D:] + term[D:].T
            suffix = term[:D] if suffix is None else suffix + term[:D]
            pairs = pair if pairs is None else pairs + pair


def finish(k, v, suffix, pairs):
    t_high, t_low = split2(suffix.T)
    weights = rows(*split2(suffix), *split2(-pairs))
    return mm(lanes(v, v, k, k), weights), mm(lanes(k, k), rows(t_high, t_low))


def last_kernel(k_ref, v_ref, state_ref, local_k_ref, local_v_ref, grad_k_ref, grad_v_ref, gain_ref):
    pairs = unpack(state_ref[D : D + 64], state_ref[D + 64 : D + 65])
    grad_k, grad_v = finish(k_ref[...], v_ref[...], state_ref[:D], pairs)
    grad_v_ref[...] = (local_v_ref[...] + grad_v).astype(BF16)
    grad_k_ref[...] = (local_k_ref[...] + grad_k).astype(BF16)
    gain_ref[...] = jnp.sum(state_ref[D + 72 : D + 80], axis=0, keepdims=True)


def exchange(array, axis):
    return lax.all_to_all(array, axis, split_axis=0, concat_axis=0, tiled=True)


def scan_over_seq(kernel, parts):
    slices = (SLICES, 8, D)
    held = exchange(parts.reshape(slices), SEQ)
    (held,) = call(kernel, [(slices, F32)], [VMEM], (held,), 10**5)
    return exchange(held, SEQ).reshape(2 * D, D)


def per_device(queries, keys, values, ridge, gain, grad_out):
    tok = queries.shape[0]
    chunks = tok // C
    token = (tok, D)
    state_shape = ((2 * D, D), F32)

    gain_row = gain.reshape(1, D)
    (parts,) = call(
        gram_kernel, [state_shape], [HBM] * 2, (keys, values), 4 * tok * D * D, grant=55000,
        scratch=[pltpu.VMEM(token, BF16), pltpu.VMEM(token, BF16), pltpu.SemaphoreType.DMA((2, 2))],
    )
    ridge_row = jnp.broadcast_to(ridge.reshape(1, 1), (1, D))
    parts, ridge_row = lax.optimization_barrier((parts, ridge_row))
    state = scan_over_seq(before_kernel, parts)
    solved, mixed, sums, wide, tall, assoc = call(
        forward_kernel,
        [(token, F32), (token, F32), ((HEADS, 8, D), F32),
         ((chunks, 2 * C, 2 * D), BF16), ((chunks, 3 * C, D), BF16), ((chunks, D, D), F32)],
        [VMEM] * 7,
        (ridge_row, gain_row, queries, keys, values, grad_out, state),
        10**9,
    )
    sums = exchange(sums, ("core", "y"))
    scaled, adjoint, grad_mixed, parts = call(
        adjoint_kernel,
        [(token, BF16), (token, F32), (token, F32), state_shape],
        [VMEM] * 10,
        (gain_row, keys, values, grad_out, sums, solved, mixed, wide, tall, assoc),
        10**9,
    )
    local_k, local_v, output, grad_q = call(
        local_kernel,
        [(token, F32), (token, F32), (token, BF16), (token, BF16)],
        [VMEM] * 6,
        (keys, values, solved, adjoint, grad_mixed, scaled),
        5 * 10**8,
    )
    state = scan_over_seq(after_kernel, parts)
    grad_k, grad_v, grad_gain = call(
        last_kernel, [(token, BF16), (token, BF16), ((1, D), F32)], [VMEM] * 5,
        (keys, values, state, local_k, local_v), 10**8,
    )
    return output, grad_q, grad_k, grad_v, grad_gain.reshape(D)


def solution(mesh):
    split = Mesh(mesh.devices.reshape(ZN, XN, mesh.shape["head"] // 2, 2), ("z", "x", "y", "core"))
    head = ("y", "core")
    tokens = P(SEQ, head)
    return jax.shard_map(
        per_device,
        mesh=split,
        in_specs=(tokens, tokens, tokens, P(head), P(head), tokens),
        out_specs=(tokens, tokens, tokens, tokens, P(head)),
        check_vma=False,
    )
```

```python
import jax
import jax.numpy as jnp
from jax import lax
from jax.experimental import pallas as pl
from jax.experimental.pallas import tpu as pltpu
from jax.sharding import Mesh
from jax.sharding import PartitionSpec as P

HEADS = 8
D = 128
CG_STEPS = 6
EPS = 1e-06
ZN = 8
XN = 4
SLICES = ZN * XN
GAIN_SLICE = 25
SEQ = ("z", "x")
C = 128
F32 = jnp.float32
BF16 = jnp.bfloat16
VMEM = pl.BlockSpec(memory_space=pltpu.VMEM)
HBM = pl.BlockSpec(memory_space=pltpu.HBM)


def split2(x):
    high = x.astype(BF16)
    return high, (x - high.astype(F32)).astype(BF16)


def mm(left, right):
    return jnp.dot(left, right, preferred_element_type=F32)


def mm_t(left, right):
    return lax.dot_general(left, right, (((0,), (0,)), ((), ())), preferred_element_type=F32)


def lanes(*parts):
    return jnp.concatenate(parts, axis=1)


def rows(*parts):
    return jnp.concatenate(parts, axis=0)


def iota2(axis):
    return lax.broadcasted_iota(jnp.int32, (C, C), axis)


def row_sum(x):
    return jnp.sum(x, axis=-1, keepdims=True)


def call(kernel, outs, ins, args, flops, grant=8192, scratch=()):
    size = sum(a.size * a.dtype.itemsize for a in args)
    return pl.pallas_call(
        kernel,
        out_shape=[jax.ShapeDtypeStruct(s, t) for s, t in outs],
        in_specs=ins,
        out_specs=[VMEM] * len(outs),
        scratch_shapes=list(scratch),
        compiler_params=pltpu.CompilerParams(vmem_limit_bytes=grant * 2**10),
        cost_estimate=pl.CostEstimate(flops=flops, bytes_accessed=size, transcendentals=0),
    )(*args)


def masked_apply(left, wide, tall, keep):
    high, low = split2(left)
    both = mm(lanes(high, low), wide)
    inner = jnp.where(keep, both[:, :C], 0.0)
    s_high, s_low = split2(inner)
    return both[:, C:] + mm(lanes(s_high, s_low, high), tall)


def conjugate(rhs, wide_ref, tall_ref, keep, exact=None, with_inner=False):
    each = range(len(rhs))
    sol = [None] * len(rhs)
    res = list(rhs)
    sea = list(rhs)
    now = [row_sum(r * r) for r in res]
    if exact is None:
        res_wide = [mm(lanes(*split2(r)), wide_ref[c]) for c, r in enumerate(res)]
    else:
        res_wide = [mm(r, wide_ref[c, :C]) for c, r in enumerate(exact)]
    sea_wide = list(res_wide)
    sol_inner = [None] * len(rhs)
    for step in range(CG_STEPS):
        last = step == CG_STEPS - 1
        image = []
        for c in each:
            inner = jnp.where(keep, sea_wide[c][:, :C], 0.0)
            s_high, s_low = split2(inner)
            image.append(sea_wide[c][:, C:] + mm(lanes(s_high, s_low, sea[c].astype(BF16)), tall_ref[c]))
        if not last:
            image_wide = [mm(lanes(*split2(image[c])), wide_ref[c]) for c in each]
        alpha = [now[c] / (row_sum(sea[c] * image[c]) + EPS) for c in each]
        sol = [alpha[c] * sea[c] if step == 0 else sol[c] + alpha[c] * sea[c] for c in each]
        if with_inner:
            inner = [alpha[c] * sea_wide[c][:, :C] for c in each]
            sol_inner = inner if step == 0 else [sol_inner[c] + inner[c] for c in each]
        if last:
            break
        res = [res[c] - alpha[c] * image[c] for c in each]
        new = [row_sum(res[c] * res[c]) for c in each]
        beta = [new[c] / (now[c] + EPS) for c in each]
        sea = [res[c] + beta[c] * sea[c] for c in each]
        res_wide = [res_wide[c] - alpha[c] * image_wide[c] for c in each]
        sea_wide = [res_wide[c] + beta[c] * sea_wide[c] for c in each]
        now = new
    return sol, sol_inner


def gram_kernel(k_hbm, v_hbm, out_ref, k_ref, v_ref, sem):
    half = k_hbm.shape[0] // 2
    at = [pl.ds(half * n, half) for n in range(2)]
    copies = [
        pltpu.make_async_copy(source.at[at[n]], target.at[at[n]], sem.at[n, m])
        for n in range(2)
        for m, (source, target) in enumerate(((k_hbm, k_ref), (v_hbm, v_ref)))
    ]
    for copy in copies:
        copy.start()
    total = None
    for n in range(2):
        copies[2 * n].wait()
        copies[2 * n + 1].wait()
        k = k_ref[at[n]]
        term = mm_t(lanes(k, v_ref[at[n]]), k)
        total = term if total is None else total + term
    out_ref[...] = total


def before_kernel(a_ref, out_ref):
    run = jnp.zeros((8, D), F32)
    for k in range(SLICES):
        out_ref[k] = run
        run = run + a_ref[k]


def after_kernel(a_ref, out_ref):
    total = a_ref[0]
    for k in range(1, SLICES):
        total = total + a_ref[k]
    whole = lax.axis_index("z") * XN + lax.axis_index("x") == GAIN_SLICE
    run = jnp.zeros((8, D), F32)
    for k in reversed(range(SLICES)):
        out_ref[k] = jnp.where(whole, total, run)
        run = run + a_ref[k]


def pack(pairs):
    row = lax.broadcasted_iota(jnp.int32, (C // 2, C), 0)
    col = lax.broadcasted_iota(jnp.int32, (C // 2, C), 1)
    turned = pltpu.roll(pairs[C // 2 :], C // 2, 1)
    return jnp.where((col < C // 2) & (col > row), turned, pairs[: C // 2])


def unpack(packed, diagonal):
    row, col = iota2(0), iota2(1)
    half = C // 2
    both = rows(packed, pltpu.roll(packed, half, 1))
    direct = ((row < half) & ((col >= half) | (row >= col))) | ((row >= half) & (col >= half) & (row < col))
    return jnp.where(row == col, diagonal, jnp.where(direct, both, both.T))


def forward_kernel(ridge_ref, gain_ref, q_ref, k_ref, v_ref, g_ref, state_ref,
                   solved_ref, mixed_ref, sums_ref, wide_ref, tall_ref, assoc_ref):
    chunks = q_ref.shape[0] // C
    each = range(chunks)
    at = [slice(C * c, C * c + C) for c in each]
    keep = iota2(0) >= iota2(1)
    eye = iota2(0) == iota2(1)
    gram = state_ref[:D] + jnp.where(eye, ridge_ref[...], 0.0)
    assoc = state_ref[D:]
    for c in each:
        k = k_ref[at[c]]
        v = v_ref[at[c]]
        k_t = k.T
        high, low = split2(gram)
        top = lanes(k_t, high)
        wide_ref[c, :C] = top
        wide_ref[c, C:] = top
        tall_ref[c] = rows(k, k, low)
        assoc_ref[c] = assoc
        if c < chunks - 1:
            more = mm(rows(k_t, v.T), k)
            gram = gram + more[:C]
            assoc = assoc + more[C:]
    weights = []
    for c in each:
        v = v_ref[at[c]]
        high, low = split2(assoc_ref[c].T)
        weights.append(rows(v, v, high, high, low))
    solved, inner = conjugate(
        [q_ref[at[c]].astype(F32) for c in each], wide_ref, tall_ref, keep, [q_ref[at[c]] for c in each], True
    )
    gain = gain_ref[...]
    ones = jnp.ones((8, 2 * D), BF16)
    for c in each:
        x_high, x_low = split2(solved[c])
        s_high, s_low = split2(jnp.where(keep, inner[c], 0.0))
        mixed = mm(lanes(s_high, s_low, x_high, x_low, x_high), weights[c])
        solved_ref[at[c]] = solved[c]
        mixed_ref[at[c]] = mixed
        square = mixed * mixed
        cross = gain * g_ref[at[c]].astype(F32) * mixed
        for n, x in enumerate((square, cross)):
            total = lax.dot_general(
                ones, lanes(*split2(x)), (((1,), (1,)), ((), ())), preferred_element_type=F32
            )
            row = 4 * n + c
            for h in range(HEADS):
                sums_ref[h, row : row + 1] = total[:1]


def adjoint_kernel(gain_ref, k_ref, v_ref, g_ref, sums_ref, solved_ref, mixed_ref, wide_ref, tall_ref, assoc_ref,
                   out_ref, adjoint_ref, grad_mixed_ref, part_ref):
    chunks = k_ref.shape[0] // C
    each = range(chunks)
    at = [slice(C * c, C * c + C) for c in each]
    keep = iota2(0) >= iota2(1)
    gain = gain_ref[...]
    sums = sums_ref[0]
    for h in range(1, HEADS):
        sums = sums + sums_ref[h]
    columns = rows(sums, jnp.zeros((C - 8, C), F32)).T
    rhs = []
    gain_part = jnp.zeros((8, D), F32)
    grads = []
    for c in each:
        denom = jnp.sqrt(columns[:, c : c + 1] / (HEADS * D) + EPS)
        inverse = 1.0 / denom
        factor = columns[:, 4 + c : 5 + c] / (denom * denom * denom * (HEADS * D))
        mixed = mixed_ref[at[c]]
        scaled = mixed * inverse
        upstream = g_ref[at[c]].astype(F32)
        out_ref[at[c]] = (scaled * gain).astype(BF16)
        gain_part = gain_part + jnp.sum((upstream * scaled).reshape(C // 8, 8, D), axis=0)
        grad = gain * upstream * inverse - mixed * factor
        grads.append(grad)
        grad_mixed_ref[at[c]] = grad
        k = k_ref[at[c]]
        high, low = split2(assoc_ref[c])
        top = lanes(v_ref[at[c]].T, high)
        rhs.append(masked_apply(grad, rows(top, top), rows(k, k, low), keep))
    turned = []
    for c in each:
        high, low = split2(solved_ref[at[c]].T)
        turned.append(lanes(high, low, high))
    part_ref[D + 72 : D + 80] = gain_part
    part_ref[D + 80 :] = jnp.zeros((D - 80, D), F32)
    adjoint, _ = conjugate(rhs, wide_ref, tall_ref, keep)
    total = None
    for c in each:
        adjoint_ref[at[c]] = adjoint[c]
        high, low = split2(lanes(grads[c], adjoint[c]))
        term = mm(turned[c], rows(high, high, low))
        total = term if total is None else total + term
    part_ref[:D] = total[:, :D]
    pairs = total[:, D:] + total[:, D:].T
    part_ref[D : D + 64] = pack(pairs)
    diagonal = jnp.sum(jnp.where(iota2(0) == iota2(1), pairs, 0.0), axis=0, keepdims=True)
    part_ref[D + 64 : D + 72] = jnp.broadcast_to(diagonal, (8, D))


def local_kernel(k_ref, v_ref, solved_ref, adjoint_ref, grad_mixed_ref, scaled_ref,
                 grad_k_ref, grad_v_ref, out_ref, grad_q_ref):
    out_ref[...] = scaled_ref[...]
    grad_q_ref[...] = adjoint_ref[...].astype(BF16)
    chunks = k_ref.shape[0] // C
    keep = iota2(0) <= iota2(1)
    suffix = pairs = None
    for c in reversed(range(chunks)):
        at = slice(C * c, C * c + C)
        k = k_ref[at]
        v = v_ref[at]
        solved, adjoint, grad = solved_ref[at], adjoint_ref[at], grad_mixed_ref[at]
        s_high, s_low = split2(solved)
        a_high, a_low = split2(adjoint)
        g_high, g_low = split2(grad)
        st_high, st_low = split2(solved.T)
        at_high, at_low = split2(adjoint.T)
        gt_high, gt_low = split2(grad.T)
        both = mm(lanes(k, k), rows(lanes(st_high, at_high), lanes(st_low, at_low)))
        value_grad = mm(lanes(v, v), rows(gt_high, gt_low))
        key_solved = jnp.where(keep, both[:, :C], 0.0)
        other = jnp.where(keep, value_grad - both[:, C:], 0.0)
        ks_high, ks_low = split2(key_solved)
        o_high, o_low = split2(other)
        grad_v = mm(lanes(ks_high, ks_low, ks_high), rows(g_high, g_high, g_low))
        grad_k = mm(lanes(o_high, o_low, o_high), rows(s_high, s_high, s_low)) - mm(
            lanes(ks_high, ks_low, ks_high), rows(a_high, a_high, a_low)
        )
        if suffix is not None:
            more_k, more_v = finish(k, v, suffix, suffix.T, pairs)
            grad_k = grad_k + more_k
            grad_v = grad_v + more_v
        grad_k_ref[at] = grad_k
        grad_v_ref[at] = grad_v
        if c > 0:
            left_high, left_low = rows(gt_high, at_high), rows(gt_low, at_low)
            term = mm(lanes(left_high, left_low, left_high), rows(s_high, s_high, s_low))
            pair = term[D:] + term[D:].T
            suffix = term[:D] if suffix is None else suffix + term[:D]
            pairs = pair if pairs is None else pairs + pair


def finish(k, v, suffix, turned, pairs):
    t_high, t_low = split2(turned)
    weights = rows(*split2(suffix), *split2(-pairs))
    return mm(lanes(v, v, k, k), weights), mm(lanes(k, k), rows(t_high, t_low))


def last_kernel(k_ref, v_ref, state_ref, local_k_ref, local_v_ref, grad_k_ref, grad_v_ref, gain_ref):
    pairs = unpack(state_ref[D : D + 64], state_ref[D + 64 : D + 65])
    turned = state_ref[:D]
    grad_k, grad_v = finish(k_ref[...], v_ref[...], turned.T, turned, pairs)
    grad_v_ref[...] = (local_v_ref[...] + grad_v).astype(BF16)
    grad_k_ref[...] = (local_k_ref[...] + grad_k).astype(BF16)
    gain_ref[...] = jnp.sum(state_ref[D + 72 : D + 80], axis=0, keepdims=True)


def exchange(array, axis):
    return lax.all_to_all(array, axis, split_axis=0, concat_axis=0, tiled=True)


def scan_over_seq(kernel, parts):
    slices = (SLICES, 8, D)
    held = exchange(parts.reshape(slices), SEQ)
    (held,) = call(kernel, [(slices, F32)], [VMEM], (held,), 10**5)
    return exchange(held, SEQ).reshape(2 * D, D)


def per_device(queries, keys, values, ridge, gain, grad_out):
    tok = queries.shape[0]
    chunks = tok // C
    token = (tok, D)
    state_shape = ((2 * D, D), F32)

    gain_row = gain.reshape(1, D)
    (parts,) = call(
        gram_kernel, [state_shape], [HBM] * 2, (keys, values), 4 * tok * D * D, grant=55000,
        scratch=[pltpu.VMEM(token, BF16), pltpu.VMEM(token, BF16), pltpu.SemaphoreType.DMA((2, 2))],
    )
    ridge_row = jnp.broadcast_to(ridge.reshape(1, 1), (1, D))
    parts, ridge_row = lax.optimization_barrier((parts, ridge_row))
    state = scan_over_seq(before_kernel, parts)
    solved, mixed, sums, wide, tall, assoc = call(
        forward_kernel,
        [(token, F32), (token, F32), ((HEADS, 8, D), F32),
         ((chunks, 2 * C, 2 * D), BF16), ((chunks, 3 * C, D), BF16), ((chunks, D, D), F32)],
        [VMEM] * 7,
        (ridge_row, gain_row, queries, keys, values, grad_out, state),
        10**9,
    )
    sums = exchange(sums, ("core", "y"))
    scaled, adjoint, grad_mixed, parts = call(
        adjoint_kernel,
        [(token, BF16), (token, F32), (token, F32), state_shape],
        [VMEM] * 10,
        (gain_row, keys, values, grad_out, sums, solved, mixed, wide, tall, assoc),
        10**9,
    )
    local_k, local_v, output, grad_q = call(
        local_kernel,
        [(token, F32), (token, F32), (token, BF16), (token, BF16)],
        [VMEM] * 6,
        (keys, values, solved, adjoint, grad_mixed, scaled),
        5 * 10**8,
    )
    state = scan_over_seq(after_kernel, parts)
    grad_k, grad_v, grad_gain = call(
        last_kernel, [(token, BF16), (token, BF16), ((1, D), F32)], [VMEM] * 5,
        (keys, values, state, local_k, local_v), 10**8,
    )
    return output, grad_q, grad_k, grad_v, grad_gain.reshape(D)


def solution(mesh):
    split = Mesh(mesh.devices.reshape(ZN, XN, mesh.shape["head"] // 2, 2), ("z", "x", "y", "core"))
    head = ("y", "core")
    tokens = P(SEQ, head)
    return jax.shard_map(
        per_device,
        mesh=split,
        in_specs=(tokens, tokens, tokens, P(head), P(head), tokens),
        out_specs=(tokens, tokens, tokens, tokens, P(head)),
        check_vma=False,
    )
```
